32 devices in a mesh: rep: 4 (over z), px: 4 (over x, core), py: 2 (over y).
Axes of the slice: x: 2, y: 2, z: 4, core: 2. Of those that a mesh axis runs over, the one named last changes fastest.
Arguments:
- state: float32 [12, 2, 192, 96, 256], P('rep', None, 'px', 'py'), parts along dimension 0, may hold values from -6 to 6
- cotangent: float32 [12, 2, 192, 96, 256], P('rep', None, 'px', 'py'), parts along dimension 0, may hold values from -6 to 6
- w_in: bfloat16 [512, 192], replicated, may hold values from -0.4375 to 0.4375
- b_in: float32 [512], replicated, may hold values from -5 to 5
- w_out: bfloat16 [192, 512], replicated, may hold values from -0.25 to 0.25
Outputs:
- state_grad: float32 [12, 2, 192, 96, 256], P('rep', None, 'px', 'py'), parts along dimension 0
- grad_in: float32 [512, 768], P(('px', 'py'), 'rep'), parts along dimension 1
- grad_out: float32 [768, 512], P('rep', ('px', 'py')), parts along dimension 0
- grad_bias: float32 [4, 512], P('rep', ('px', 'py')), parts along dimension 0
The draws below stay inside these ranges and needn't reach their ends.
There are 4 independent parts, one for each index of `rep`. The reference program is written for one: setup_inputs(seed, part) draws one part's arguments, and reference() takes and returns one part's arrays. A program takes and returns all parts, laid end to end along the dimension named above; an argument that names none is the same for every part. Nothing has to cross between parts.
All inputs are finite; a program needn't handle non-finite values.
Results may differ from the reference program's by a relative error of at most 0.0065.
The reference program's roundings to bfloat16 on the way count: a program that leaves them out, or rounds other values in their place, can miss the bound.
Values may be sent and summed in bfloat16 or wider, within the bound.
No kernel may reach another device: no remote copies, remote signals or barrier semaphores. Data moves between devices by JAX's collectives and lax.ppermute only.
A program may use at most 448 MiB of HBM per device.

```python
import math
import jax
import jax.numpy as jnp
from jax import lax

NG = 256
KY = 192
KZ = 96
PATCH = 4
FEAT = 192
HID = 512


def steps_of(rng, shape, cuts, smallest, largest):
    def one(position, blocks):
        heights = jax.random.uniform(jax.random.fold_in(jax.random.fold_in(rng, 6), position), (blocks,), jnp.float32, smallest / len(cuts), largest / len(cuts))
        return jnp.repeat(jnp.exp(heights), shape[position] // blocks).reshape((-1,) + (1,) * (len(shape) - position - 1))

    level = one(*cuts[0])
    for cut in cuts[1:]:
        level = level * one(*cut)
    return level


def centred(rng, dims, deviation, reach, pieces=(), held_as=jnp.bfloat16):
    drawn = jax.random.normal(rng, dims, jnp.float32) * deviation
    if len(pieces) > 0:
        drawn = steps_of(rng, dims, pieces, -0.22, 0.18) * drawn
    return jnp.clip(drawn, min=-reach, max=reach).astype(held_as)


def setup_inputs(seed: int = 0, part: int = 0) -> dict:
    seeds = jax.random.split(jax.random.key(seed), 6)
    own_keys = jax.random.split(jax.random.fold_in(seeds[5], part), 6)
    state = centred(own_keys[0], (3, 2, KY, KZ, NG), 1.3, 6.0, ((2, 4), (3, 2)), jnp.float32)
    cotangent = centred(own_keys[1], (3, 2, KY, KZ, NG), 1.0, 6.0, ((2, 4), (3, 2)), jnp.float32)
    w_in = centred(seeds[2], (HID, FEAT), FEAT ** -0.5, 0.4375)
    b_in = centred(seeds[3], (HID,), 1.0, 5.0, (), jnp.float32)
    w_out = centred(seeds[4], (FEAT, HID), HID ** -0.5, 0.25)
    return dict(state=state, cotangent=cotangent, w_in=w_in, b_in=b_in, w_out=w_out)


NU_DT = 5e-05
TIME_STEP = 0.01
FORCING = 20.0

def angles(leading, trailing, length):
    product = leading[:, None] * trailing[None, :] % length
    phases = product.astype(jnp.float32) * (2.0 * math.pi / length)
    factor = 1.0 / math.sqrt(length)
    return (jnp.cos(phases) * factor, jnp.sin(phases) * factor)

def mode_ids(count, length):
    counter = jnp.arange(count, dtype=jnp.int32)
    return jnp.where(counter < count // 2, counter, counter + length - count).astype(jnp.int32)

def mode_table(modes, length, direction):
    cosine, sine_part = angles(modes, jnp.arange(length, dtype=jnp.int32), length)
    top_rows = jnp.stack([cosine, direction * sine_part], axis=1)
    low_rows = jnp.stack([-direction * sine_part, cosine], axis=1)
    return jnp.stack([top_rows, low_rows], axis=0).astype(jnp.bfloat16)

def complex_table(length, direction):
    return mode_table(jnp.arange(length, dtype=jnp.int32), length, direction)

def real_table(length, mode_count):
    cosine, sine_part = angles(jnp.arange(mode_count, dtype=jnp.int32), jnp.arange(length, dtype=jnp.int32), length)
    return jnp.stack([cosine, -sine_part], axis=0).astype(jnp.bfloat16)

def rounded(values):
    return lax.optimization_barrier(values.astype(jnp.bfloat16)).astype(jnp.float32)

def signed(counter, length):
    return jnp.where(counter < length // 2, counter, counter - length).astype(jnp.float32)

def factors(ky_ids, kz_ids, length, ky_count):
    cutoff = length // 3
    wave_y = signed(ky_ids, ky_count)[:, None, None]
    wave_z = kz_ids.astype(jnp.float32)[None, :, None]
    wave_x = signed(jnp.arange(length, dtype=jnp.int32), length)[None, None, :]
    retained = ((jnp.abs(wave_x) <= cutoff) & (jnp.abs(wave_y) <= cutoff) & (wave_z <= cutoff)).astype(jnp.float32)
    square = wave_x * wave_x + wave_y * wave_y + wave_z * wave_z
    damping = jnp.exp(-NU_DT * square)
    weight = jnp.where(kz_ids[None, :, None] == 0, 1.0, 2.0).astype(jnp.float32)
    return ((wave_x, wave_y, wave_z), retained, damping, weight, square)

def cross(former, latter):
    return [former[1] * latter[2] - former[2] * latter[1], former[2] * latter[0] - former[0] * latter[2], former[0] * latter[1] - former[1] * latter[0]]

def curl_modes(waves, spectra):
    real_part = cross(waves, [spectra[slot, 0] for slot in range(3)])
    imag_part = cross(waves, [spectra[slot, 1] for slot in range(3)])
    return jnp.stack([jnp.stack([-imag_part[slot], real_part[slot]]) for slot in range(3)])

def project(waves, square, spectra):
    dotted = waves[0] * spectra[0] + waves[1] * spectra[1] + waves[2] * spectra[2]
    along_k = dotted / jnp.maximum(square, 1.0)
    return jnp.stack([spectra[slot] - waves[slot] * along_k for slot in range(3)])

def to_physical(spectra):
    length = spectra.shape[4]
    inverse = complex_table(length, 1.0).astype(jnp.float32)
    y_inverse = mode_table(mode_ids(spectra.shape[2], length), length, 1.0).astype(jnp.float32)
    z_table = real_table(length, spectra.shape[3]).astype(jnp.float32)
    sectioned = rounded(spectra)
    sectioned = rounded(jnp.einsum('cramn,rnsx->csamx', sectioned, inverse, precision=lax.Precision.HIGHEST))
    sectioned = rounded(jnp.einsum('csamx,saty->ctmxy', sectioned, y_inverse, precision=lax.Precision.HIGHEST))
    return jnp.einsum('ctmxy,tmz->cxyz', sectioned, z_table, precision=lax.Precision.HIGHEST).astype(jnp.bfloat16)

def to_spectral(field):
    length = field.shape[3]
    forward = complex_table(length, -1.0).astype(jnp.float32)
    y_forward = mode_table(mode_ids(KY, length), length, -1.0).astype(jnp.float32).transpose(0, 3, 2, 1)
    z_table = real_table(length, KZ).astype(jnp.float32)
    sectioned = field.astype(jnp.float32)
    sectioned = rounded(jnp.einsum('cxyz,rmz->crmxy', sectioned, z_table, precision=lax.Precision.HIGHEST))
    sectioned = rounded(jnp.einsum('crmxy,rysa->csamx', sectioned, y_forward, precision=lax.Precision.HIGHEST))
    return jnp.einsum('csamx,sxtn->ctamn', sectioned, forward, precision=lax.Precision.HIGHEST)

def to_boxes(field):
    channels, span_x, span_y, span_z = field.shape
    tiles = field.reshape(channels, span_x // PATCH, PATCH, span_y // PATCH, PATCH, span_z // PATCH, PATCH)
    return tiles.transpose(0, 2, 4, 6, 1, 3, 5).reshape(channels * PATCH ** 3, -1)

def from_boxes(box_values, layout):
    channels, span_x, span_y, span_z = layout
    tiles = box_values.reshape(channels, PATCH, PATCH, PATCH, span_x // PATCH, span_y // PATCH, span_z // PATCH)
    return tiles.transpose(0, 4, 1, 5, 2, 6, 3).reshape(layout)

def closure_terms(velocity, force_adj, w_in, b_in, w_out):
    features = to_boxes(velocity)
    adjoints = to_boxes(force_adj)
    pre_act = jnp.dot(w_in, features, preferred_element_type=jnp.float32) + b_in[:, None]
    hidden = jax.nn.silu(pre_act).astype(jnp.bfloat16)
    sigmoid = jax.nn.sigmoid(pre_act)
    hidden_adj = FORCING * jnp.dot(w_out.T, adjoints, preferred_element_type=jnp.float32)
    pre_adj = (hidden_adj * sigmoid * (1.0 + pre_act * (1.0 - sigmoid))).astype(jnp.bfloat16)
    grad_in = jnp.dot(pre_adj, features.T, preferred_element_type=jnp.float32)
    grad_out = FORCING * jnp.dot(adjoints, hidden.T, preferred_element_type=jnp.float32)
    grad_bias = lax.optimization_barrier(jnp.sum(pre_adj.astype(jnp.float32), axis=1))[None, :]
    feat_adj = jnp.dot(w_in.T, pre_adj, preferred_element_type=jnp.float32)
    return (from_boxes(feat_adj, velocity.shape), grad_in, grad_out, grad_bias)

def pointwise(feat_adj, velocity, vorticity, force_adj):
    vel_list = [velocity[slot].astype(jnp.float32) for slot in range(3)]
    vort_list = [vorticity[slot].astype(jnp.float32) for slot in range(3)]
    force_list = [force_adj[slot].astype(jnp.float32) for slot in range(3)]
    turned = cross(vort_list, force_list)
    vel_adj = jnp.stack([feat_adj[slot] + turned[slot] for slot in range(3)]).astype(jnp.bfloat16)
    vort_adj = jnp.stack(cross(force_list, vel_list)).astype(jnp.bfloat16)
    return (vel_adj, vort_adj)

def reference(state, cotangent, w_in, b_in, w_out):
    waves, retained, damping, weight, square = factors(jnp.arange(KY, dtype=jnp.int32), jnp.arange(KZ, dtype=jnp.int32), NG, KY)
    kept = retained * state
    spectra = weight * jnp.concatenate([kept, curl_modes(waves, kept)], axis=0)
    fields = to_physical(spectra)
    velocity, vorticity = (fields[:3], fields[3:])
    force_spec = TIME_STEP * retained * project(waves, square, damping * cotangent)
    force_adj = to_physical(force_spec)
    feat_adj, grad_in, grad_out, grad_bias = closure_terms(velocity, force_adj, w_in, b_in, w_out)
    vel_adj, vort_adj = pointwise(feat_adj, velocity, vorticity, force_adj)
    spectral = to_spectral(jnp.concatenate([vel_adj, vort_adj], axis=0))
    state_grad = damping * cotangent + weight * retained * (spectral[:3] + curl_modes(waves, spectral[3:]))
    return (state_grad, grad_in, grad_out, grad_bias)
```

```python
import functools
import math

import jax
import jax.numpy as jnp
from jax import lax
from jax.experimental import pallas as pl
from jax.experimental.pallas import tpu as pltpu
from jax.sharding import PartitionSpec as P

PATCH = 4
NU_DT = 5e-05
TIME_STEP = 0.01
FORCING = 20.0
LANES = 128
F32 = jnp.float32
BF16 = jnp.bfloat16

OUT_SLOTS = ("uy", "uz", "ux", "wy", "wz", "fx", "fy", "fz")
BACK_SLOTS = ("ax", "az", "gy", "gz", "ay")


def up_to(value, step):
    return -(-value // step) * step


def angles(leading, trailing, length):
    product = leading[:, None] * trailing[None, :] % length
    phases = product.astype(F32) * (2.0 * math.pi / length)
    factor = 1.0 / math.sqrt(length)
    return jnp.cos(phases) * factor, jnp.sin(phases) * factor


def mode_ids(count, length):
    counter = jnp.arange(count, dtype=jnp.int32)
    return jnp.where(counter < count // 2, counter, counter + length - count)


def box_order(length):
    counter = jnp.arange(length, dtype=jnp.int32)
    boxes = length // PATCH
    return counter % boxes * PATCH + counter // boxes


def signed(counter, length):
    return jnp.where(counter < length // 2, counter, counter - length).astype(F32)


def dot(a, b):
    return lax.dot_general(a, b, (((1,), (0,)), ((), ())), preferred_element_type=F32)


def dot_nt(a, b):
    return lax.dot_general(a, b, (((1,), (1,)), ((), ())), preferred_element_type=F32)


def dot_tn(a, b):
    return lax.dot_general(a, b, (((0,), (0,)), ((), ())), preferred_element_type=F32)


def lane_modes(slot, width_z, lanes, first):
    local = jnp.arange(lanes, dtype=jnp.int32) - slot * width_z
    inside = (local >= 0) & (local < width_z)
    return jnp.where(inside, local, 0) + first, inside


def vregs_of(slot, width_z):
    return list(range(slot * width_z // LANES, ((slot + 1) * width_z - 1) // LANES + 1))


def spectra_kernel(ky_ref, kz_ref, state_ref, cot_ref, out_ref, *, block, length):
    cutoff = float(length // 3)
    wave_z = kz_ref[...]
    counter = lax.broadcasted_iota(jnp.int32, wave_z.shape, 1)
    wave_x = jnp.where(counter < length // 2, counter, counter - length).astype(F32)
    plane = wave_x * wave_x + wave_z * wave_z
    inside = (jnp.abs(wave_x) <= cutoff) & (wave_z <= cutoff)
    weight = jnp.where(wave_z == 0.0, 1.0, 2.0).astype(F32)
    base = pl.program_id(0) * block

    def one(k, carry):
        wave_y = ky_ref[base + k]
        kept = jnp.where(inside & (jnp.abs(wave_y) <= cutoff), 1.0, 0.0).astype(F32)
        square = plane + wave_y * wave_y
        damped = jnp.exp(-NU_DT * square)
        scale = kept * weight
        push = kept * damped * TIME_STEP
        inverse = 1.0 / jnp.maximum(square, 1.0)
        u = [[scale * state_ref[c, r, k] for r in range(2)] for c in range(3)]
        for r in range(2):
            lanes = pl.ds(r * length, length)
            g = [push * cot_ref[c, r, k] for c in range(3)]
            along = (wave_x * g[0] + wave_y * g[1] + wave_z * g[2]) * inverse
            sign = -1.0 if r == 0 else 1.0
            q = 1 - r
            wy = sign * (wave_z * u[0][q] - wave_x * u[2][q])
            wz = sign * (wave_x * u[1][q] - wave_y * u[0][q])
            fx = g[0] - wave_x * along
            fy = g[1] - wave_y * along
            fz = g[2] - wave_z * along
            rows = (u[1][r], u[2][r], u[0][r], wy, wz, fx, fy, fz)
            for slot, value in enumerate(rows):
                out_ref[k, slot, :, lanes] = value.astype(BF16)
        return carry

    lax.fori_loop(0, block, one, 0)


def make_spectra(ky, kz_col, state, cotangent):
    _, _, width_y, width_z, length = state.shape
    block = 8
    slots = len(OUT_SLOTS)
    spec = pl.BlockSpec((3, 2, block, width_z, length), lambda i: (0, 0, i, 0, 0))
    return pl.pallas_call(
        functools.partial(spectra_kernel, block=block, length=length),
        grid=(width_y // block,),
        in_specs=[
            pl.BlockSpec(memory_space=pltpu.SMEM),
            pl.BlockSpec((width_z, length), lambda i: (0, 0)),
            spec,
            spec,
        ],
        out_specs=pl.BlockSpec((block, slots, width_z, 2 * length), lambda i: (i, 0, 0, 0)),
        out_shape=jax.ShapeDtypeStruct((width_y, slots, width_z, 2 * length), BF16),
        compiler_params=pltpu.CompilerParams(vmem_limit_bytes=56 * 2**20),
        name="spectra",
    )(ky, kz_col, state, cotangent)


def along_x_kernel(table_ref, spec_ref, out_ref, scratch, *, block, rows, width_y, span):
    step = pl.program_id(0)
    lanes = out_ref.shape[3]
    table = table_ref[...]
    live = spec_ref.shape[1]

    def one(k, carry):
        value = dot_nt(table, spec_ref[k])
        start = pl.multiple_of((step * block + k) * rows, 8)
        for v in range(lanes // LANES):
            if (v + 1) * LANES <= live:
                piece = value[:, v * LANES : (v + 1) * LANES]
                scratch[v, pl.ds(start, rows), :] = piece
            else:
                scratch[v, pl.ds(start, rows), :] = jnp.zeros((rows, LANES), F32)
                scratch[v, pl.ds(start, rows), pl.ds(0, live - v * LANES)] = value[:, v * LANES :]
        return carry

    lax.fori_loop(0, block, one, 0)

    @pl.when(step == pl.num_programs(0) - 1)
    def _():
        def move(i, carry):
            dest = i // span
            x = i % span
            for v in range(lanes // LANES):
                parts = [scratch[v, pl.ds(2 * i + s, width_y, stride=rows), :] for s in range(2)]
                block_rows = jnp.concatenate(parts, axis=0).astype(BF16)
                out_ref[dest, x, :, pl.ds(v * LANES, LANES)] = block_rows
            return carry

        lax.fori_loop(0, rows // 2, move, 0)


def along_x(table, spectra, parts, span):
    width_y, live, depth = spectra.shape
    rows = table.shape[0]
    block = 8
    lanes = up_to(live, LANES)
    shape = (parts, span, 2 * width_y, lanes)
    return pl.pallas_call(
        functools.partial(along_x_kernel, block=block, rows=rows, width_y=width_y, span=span),
        grid=(width_y // block,),
        in_specs=[
            pl.BlockSpec((rows, depth), lambda i: (0, 0)),
            pl.BlockSpec((block, live, depth), lambda i: (i, 0, 0)),
        ],
        out_specs=pl.BlockSpec(shape, lambda i: (0, 0, 0, 0)),
        out_shape=jax.ShapeDtypeStruct(shape, BF16),
        scratch_shapes=[pltpu.VMEM((lanes // LANES, width_y * rows, LANES), F32)],
        compiler_params=pltpu.CompilerParams(vmem_limit_bytes=56 * 2**20),
        cost_estimate=pl.CostEstimate(
            flops=2 * rows * live * depth * width_y * 2,
            bytes_accessed=2 * (width_y * live * depth + rows * width_y * lanes),
            transcendentals=0,
        ),
        name="along_x",
    )(table, spectra)


def halves(low, high):
    left = lax.broadcasted_iota(jnp.int32, low.shape, 1) < LANES // 2
    turned_high = pltpu.roll(high, LANES // 2, 1)
    turned_low = pltpu.roll(low, LANES // 2, 1)
    return jnp.where(left, low, turned_high), jnp.where(left, turned_low, high)


def physical_kernel(
    recv_ref,
    ky_ref,
    kz_in_ref,
    kz_back_ref,
    ty_ref,
    tyb_ref,
    w_in_ref,
    w_in_t_ref,
    w_out_t_ref,
    bias_ref,
    *refs,
    parts_x,
    parts_y,
    width_y,
    width_z,
    length,
    back_lanes,
):
    z_refs = dict(zip(("uy", "uz", "ux", "wy", "wz", "fx", "fy", "fz", "wx"), refs[:9]))
    zb_ref = refs[9]
    out_ref, gin_ref, gout_ref = refs[10:13]
    mid, vel, force, vort, fadj, back = refs[13:]
    rows = 2 * width_y
    in_lanes = recv_ref.shape[3]
    boxes = length // PATCH
    feats = 3 * PATCH * PATCH

    @pl.when(pl.program_id(0) == 0)
    def _():
        gin_ref[...] = jnp.zeros(gin_ref.shape, F32)
        gout_ref[...] = jnp.zeros(gout_ref.shape, F32)

    def section_y(dx, carry):
        for py in range(parts_y):
            whole = jnp.concatenate(
                [recv_ref[px * parts_y + py, dx] for px in range(parts_x)], axis=0
            )
            first = whole[:, :LANES].astype(F32)
            second = pltpu.roll(first, LANES - width_z, 1)
            mixed = ky_ref[...] * second - kz_in_ref[py : py + 1, :] * first
            turned = []
            for px in range(parts_x):
                turned.append(-mixed[px * rows + width_y : (px + 1) * rows])
                turned.append(mixed[px * rows : px * rows + width_y])
            extra = jnp.concatenate(turned, axis=0).astype(BF16)
            mid[py, dx, :, pl.ds(0, in_lanes)] = dot(ty_ref[...], whole).astype(BF16)
            mid[py, dx, :, pl.ds(in_lanes, LANES)] = dot(ty_ref[...], extra).astype(BF16)
        return carry

    lax.fori_loop(0, PATCH, section_y, 0)

    def section_z(dx, carry):
        def field(name):
            if name == "wx":
                vregs = [in_lanes // LANES]
            else:
                vregs = vregs_of(OUT_SLOTS.index(name), width_z)
            pieces = [
                mid[py, dx, pl.ds(t * length, length), pl.ds(v * LANES, LANES)]
                for py in range(parts_y)
                for t in range(2)
                for v in vregs
            ]
            return dot(jnp.concatenate(pieces, axis=1), z_refs[name][...])

        for slot, name in enumerate("xyz"):
            at = pl.multiple_of((slot * PATCH + dx) * length, length)
            rows_here = pl.ds(at, length)
            for target, kind in ((vel, "u"), (force, "f")):
                value = field(kind + name).astype(BF16).astype(F32)
                for half in range(length // LANES):
                    target[half, rows_here, :] = value[:, half * LANES : (half + 1) * LANES]
            vort[rows_here, :] = field("w" + name).astype(BF16)
        return carry

    lax.fori_loop(0, PATCH, section_z, 0)

    pair = 2

    def gather(source, by):
        per_dz = []
        for half in range(2):
            got = [source[half, pl.ds(by + i, feats, stride=boxes), :] for i in range(2 * pair)]
            one = halves(got[0], got[1])
            two = halves(got[2], got[3])
            per_dz.append(jnp.concatenate([one[0], two[0]], axis=1))
            per_dz.append(jnp.concatenate([one[1], two[1]], axis=1))
        return jnp.concatenate(per_dz, axis=0).astype(BF16)

    def closure(step, carry):
        by = step * 2 * pair
        features = gather(vel, by)
        adjoints = gather(force, by)
        pre = dot(w_in_ref[...], features) + bias_ref[...]
        sigma = 0.5 * jnp.tanh(0.5 * pre) + 0.5
        hidden = (pre * sigma).astype(BF16)
        hidden_adj = FORCING * dot(w_out_t_ref[...], adjoints)
        pre_adj = (hidden_adj * sigma * (1.0 + pre * (1.0 - sigma))).astype(BF16)
        ones = jnp.ones((gin_ref.shape[1] - features.shape[0], features.shape[1]), BF16)
        gin_ref[...] += dot_nt(pre_adj, jnp.concatenate([features, ones], axis=0))
        gout_ref[...] += dot_nt(hidden, adjoints)
        back_feat = dot(w_in_t_ref[...], pre_adj)
        for half in range(2):
            low = back_feat[(2 * half) * feats : (2 * half + 1) * feats]
            high = back_feat[(2 * half + 1) * feats : (2 * half + 2) * feats]
            for p in range(2):
                cut = slice(p * LANES, (p + 1) * LANES)
                for i, value in enumerate(halves(low[:, cut], high[:, cut])):
                    fadj[half, pl.ds(by + 2 * p + i, feats, stride=boxes), :] = value
        return carry

    lax.fori_loop(0, boxes // (2 * pair), closure, 0)

    back_vregs = back_lanes // LANES

    def section_back(dx, carry):
        def rows_at(slot):
            return pl.ds(pl.multiple_of((slot * PATCH + dx) * length, length), length)

        def read(source, slot):
            return jnp.concatenate(
                [source[half, rows_at(slot), :] for half in range(length // LANES)], axis=1
            )

        u = [read(vel, c) for c in range(3)]
        f = [read(force, c) for c in range(3)]
        w = [vort[rows_at(c), :].astype(F32) for c in range(3)]
        named = {}
        for c, name in enumerate("xyz"):
            a, b = (c + 1) % 3, (c + 2) % 3
            turned = read(fadj, c) + (w[a] * f[b] - w[b] * f[a])
            named["v" + name] = turned.astype(BF16)
            named["g" + name] = (f[a] * u[b] - f[b] * u[a]).astype(BF16)
        at = 0
        for group, names in enumerate(back_groups(width_z)):
            joined = jnp.concatenate([named[name] for name in names], axis=1)
            depth = joined.shape[1]
            for py in range(parts_y):
                value = dot(joined, zb_ref[py, pl.ds(at, depth), :]).astype(BF16)
                for r in range(2):
                    piece = value[:, r * LANES : (r + 1) * LANES]
                    back[py, pl.ds(r * length, length), pl.ds(group * LANES, LANES)] = piece
            at += depth
        for py in range(parts_y):
            value = dot(tyb_ref[...], back[py])
            by_y = ky_ref[...] * value[:, back_lanes : back_lanes + LANES]
            by_z = value[:, back_lanes + LANES :]
            extra = []
            for v in range(back_vregs):
                here = kz_back_ref[py, v : v + 1, :] * by_z
                if v == 0:
                    here = here + by_y
                extra.append(here)
            extra = jnp.concatenate(extra, axis=1)
            for px in range(parts_x):
                re = slice(px * rows, px * rows + width_y)
                im = slice(px * rows + width_y, (px + 1) * rows)
                total = jnp.concatenate(
                    [value[re, :back_lanes] - extra[im], value[im, :back_lanes] + extra[re]], axis=0
                )
                out_ref[px * parts_y + py, dx] = total.astype(BF16)
        return carry

    lax.fori_loop(0, PATCH, section_back, 0)


def back_groups(width_z):
    names = [{"a": "v", "g": "g"}[slot[0]] + slot[1] for slot in BACK_SLOTS]
    lanes = up_to(len(BACK_SLOTS) * width_z, LANES)
    groups = []
    for v in range(lanes // LANES):
        groups.append([n for slot, n in enumerate(names) if v in vregs_of(slot, width_z)])
    groups.append(["gz", "gx"])
    groups.append(["gy", "gx"])
    return groups


def back_table(width_z, length, parts_y):
    names = [{"a": "v", "g": "g"}[slot[0]] + slot[1] for slot in BACK_SLOTS]
    lanes = up_to(len(BACK_SLOTS) * width_z, LANES)
    groups = back_groups(width_z)
    order = box_order(length)

    def piece(slot, vreg, py, sign):
        modes, inside = lane_modes(slot, width_z, lanes, py * width_z)
        cut = slice(vreg * LANES, (vreg + 1) * LANES)
        cosine, sine = angles(order, modes[cut], length)
        keep = sign * inside[cut].astype(F32)[None, :]
        return jnp.concatenate([cosine * keep, -sine * keep], axis=1)

    ky_slots = {"gz": (BACK_SLOTS.index("ax"), 1.0), "gx": (BACK_SLOTS.index("az"), -1.0)}
    kz_slots = {"gy": (BACK_SLOTS.index("ax"), -1.0), "gx": (BACK_SLOTS.index("ay"), 1.0)}
    tables = []
    for py in range(parts_y):
        rows = []
        for v, group in enumerate(groups[:-2]):
            rows += [piece(names.index(n), v, py, 1.0) for n in group]
        for which, group in ((ky_slots, groups[-2]), (kz_slots, groups[-1])):
            for n in group:
                slot, sign = which[n]
                rows.append(sum(piece(slot, v, py, sign) for v in vregs_of(slot, width_z)))
        tables.append(jnp.concatenate(rows, axis=0))
    return jnp.stack(tables).astype(BF16)


def out_table(slot, width_z, length, parts_y):
    lanes = (vregs_of(slot, width_z)[-1] + 1) * LANES
    order = box_order(length)
    rows = []
    for py in range(parts_y):
        modes, inside = lane_modes(slot, width_z, lanes, py * width_z)
        cosine, sine = angles(modes, order, length)
        keep = inside.astype(F32)[:, None]
        for value in (cosine, -sine):
            for v in vregs_of(slot, width_z):
                rows.append((value * keep)[v * LANES : (v + 1) * LANES])
    return jnp.concatenate(rows, axis=0).astype(BF16)


def physical(recv, ky_rows, kz_in, kz_back, tables, weights, grid_sizes, back_lanes):
    parts_x, parts_y, width_y, width_z, length = grid_sizes
    parts, span, rows, in_lanes = recv.shape
    hid = weights[0].shape[0]
    feat = weights[0].shape[1]
    t_y, t_yb, z_tables, z_back = tables

    def whole(array):
        return pl.BlockSpec(array.shape, lambda i: (0,) * array.ndim)

    small = [ky_rows, kz_in, kz_back, t_y, t_yb, *weights, *z_tables, z_back]
    feat_pad = up_to(feat + 1, 2 * LANES)
    field = (3 * PATCH * length, length)
    split = (length // LANES, 3 * PATCH * length, LANES)
    flops = 2 * span * parts_y * (2 * length) * (parts_x * rows) * (in_lanes + LANES)
    flops += 2 * 5 * hid * feat * (span * length * length // PATCH**3)
    flops += 2 * span * length * length * length * (9 * 2 + 20)
    return pl.pallas_call(
        functools.partial(
            physical_kernel,
            parts_x=parts_x,
            parts_y=parts_y,
            width_y=width_y,
            width_z=width_z,
            length=length,
            back_lanes=back_lanes,
        ),
        grid=(span // PATCH,),
        in_specs=[pl.BlockSpec((parts, PATCH, rows, in_lanes), lambda i: (0, i, 0, 0))]
        + [whole(a) for a in small],
        out_specs=[
            pl.BlockSpec((parts, PATCH, rows, back_lanes), lambda i: (0, i, 0, 0)),
            pl.BlockSpec((hid, feat_pad), lambda i: (0, 0)),
            pl.BlockSpec((hid, feat), lambda i: (0, 0)),
        ],
        out_shape=[
            jax.ShapeDtypeStruct((parts, span, rows, back_lanes), BF16),
            jax.ShapeDtypeStruct((hid, feat_pad), F32),
            jax.ShapeDtypeStruct((hid, feat), F32),
        ],
        scratch_shapes=[
            pltpu.VMEM((parts_y, PATCH, 2 * length, in_lanes + LANES), BF16),
            pltpu.VMEM(split, F32),
            pltpu.VMEM(split, F32),
            pltpu.VMEM(field, BF16),
            pltpu.VMEM(split, F32),
            pltpu.VMEM((parts_y, 2 * length, back_lanes + 2 * LANES), BF16),
        ],
        compiler_params=pltpu.CompilerParams(vmem_limit_bytes=58 * 2**20),
        cost_estimate=pl.CostEstimate(
            flops=flops, bytes_accessed=2 * recv.size * 2, transcendentals=0
        ),
        name="physical",
    )(recv, *small)


def final_kernel(
    ky_ref, kz_ref, table_ref, cot_ref, *refs, steps_in, block, chunks, span, parts, width_y, width_z, length
):
    recv_refs = refs[:chunks]
    out_ref, scratch, turned = refs[chunks:]
    step = pl.program_id(0)
    rows = 2 * width_y
    lanes = recv_refs[0].shape[3]

    @pl.when(step < steps_in)
    def _():
        for j in range(chunks):
            def load(x, carry):
                at = ((step * chunks + j) * span + x) * rows
                value = recv_refs[j][0, x].astype(F32)
                for v in range(lanes // LANES):
                    cut = value[:, v * LANES : (v + 1) * LANES]
                    scratch[v, pl.ds(pl.multiple_of(at, 8), rows), :] = cut
                return carry

            lax.fori_loop(0, span, load, 0)

    @pl.when(step >= steps_in)
    def _():
        cutoff = float(length // 3)
        wave_z = kz_ref[...]
        counter = lax.broadcasted_iota(jnp.int32, wave_z.shape, 1)
        wave_x = jnp.where(counter < length // 2, counter, counter - length).astype(F32)
        plane = wave_x * wave_x + wave_z * wave_z
        inside = (jnp.abs(wave_x) <= cutoff) & (wave_z <= cutoff)
        weight = jnp.where(wave_z == 0.0, 1.0, 2.0).astype(F32)

        def one(k, carry):
            ky = (step - steps_in) * block + k
            pieces = []
            for v in range(lanes // LANES):
                parts_s = [
                    scratch[v, pl.ds(ky + s * width_y, length, stride=rows), :] for s in range(2)
                ]
                pieces.append(jnp.concatenate(parts_s, axis=0))
            gathered = jnp.concatenate(pieces, axis=1).astype(BF16)
            turned[...] = dot_tn(gathered, table_ref[...])
            wave_y = ky_ref[ky]
            kept = jnp.where(inside & (jnp.abs(wave_y) <= cutoff), 1.0, 0.0).astype(F32)
            damped = jnp.exp(-NU_DT * (plane + wave_y * wave_y))
            scale = kept * weight

            def part(name, t):
                at = BACK_SLOTS.index(name) * width_z
                return turned[pl.ds(at, width_z), pl.ds(t * length, length)]

            for t in range(2):
                sign = -1.0 if t == 0 else 1.0
                ax = part("ax", t)
                ay = part("ay", t) - sign * wave_x * part("gz", 1 - t)
                az = part("az", t) + sign * wave_x * part("gy", 1 - t)
                for c, value in enumerate((ax, ay, az)):
                    out_ref[c, t, k] = damped * cot_ref[c, t, k] + scale * value
            return carry

        lax.fori_loop(0, block, one, 0)


def finish(ky, kz_col, table, cotangent, received):
    _, _, width_y, width_z, length = cotangent.shape
    parts, span, rows, lanes = received[0].shape
    chunks = len(received)
    block = 8
    steps_in = parts
    steps = steps_in + width_y // block
    spec = pl.BlockSpec(
        (3, 2, block, width_z, length), lambda i: (0, 0, jnp.maximum(i - steps_in, 0), 0, 0)
    )
    recv_spec = pl.BlockSpec(
        (1, span, rows, lanes), lambda i: (jnp.minimum(i, steps_in - 1), 0, 0, 0)
    )
    return pl.pallas_call(
        functools.partial(
            final_kernel,
            steps_in=steps_in,
            block=block,
            chunks=chunks,
            span=span,
            parts=parts,
            width_y=width_y,
            width_z=width_z,
            length=length,
        ),
        grid=(steps,),
        in_specs=[
            pl.BlockSpec(memory_space=pltpu.SMEM),
            pl.BlockSpec((width_z, length), lambda i: (0, 0)),
            pl.BlockSpec(table.shape, lambda i: (0, 0)),
            spec,
        ]
        + [recv_spec] * chunks,
        out_specs=spec,
        out_shape=jax.ShapeDtypeStruct(cotangent.shape, F32),
        scratch_shapes=[
            pltpu.VMEM((lanes // LANES, length * rows, LANES), F32),
            pltpu.VMEM((lanes, 2 * length), F32),
        ],
        compiler_params=pltpu.CompilerParams(vmem_limit_bytes=60 * 2**20),
        name="finish",
    )(ky, kz_col, table, cotangent, *received)


def shards(state, cotangent, w_in, b_in, w_out):
    width_y, width_z, length = state.shape[2:]
    parts_x = lax.axis_size("px")
    parts_y = lax.axis_size("py")
    parts = parts_x * parts_y
    slab = length // parts
    chunks = 4
    while chunks > 1 and slab % (chunks * PATCH) != 0:
        chunks //= 2
    span = slab // chunks
    ky_count = width_y * parts_x
    hid, feat = w_in.shape

    ky_ids = lax.axis_index("px") * width_y + jnp.arange(width_y, dtype=jnp.int32)
    kz_ids = lax.axis_index("py") * width_z + jnp.arange(width_z, dtype=jnp.int32)
    ky = signed(ky_ids, ky_count)
    kz_col = jnp.broadcast_to(kz_ids.astype(F32)[:, None], (width_z, length))

    everything = jnp.arange(length, dtype=jnp.int32)
    cosine, sine = angles(everything, everything, length)
    x_rows = jnp.stack(
        [jnp.concatenate([cosine, -sine], axis=1), jnp.concatenate([sine, cosine], axis=1)], axis=1
    ).astype(BF16)
    x_rows = x_rows.reshape(parts, chunks, span, 2, 2 * length)

    order = box_order(length)
    cosine_y, sine_y = angles(order, mode_ids(ky_count, length), length)
    cosine_y = cosine_y.reshape(length, parts_x, 1, width_y)
    sine_y = sine_y.reshape(length, parts_x, 1, width_y)
    t_y = jnp.concatenate(
        [
            jnp.concatenate([cosine_y, -sine_y], axis=2).reshape(length, -1),
            jnp.concatenate([sine_y, cosine_y], axis=2).reshape(length, -1),
        ],
        axis=0,
    ).astype(BF16)
    t_yb = t_y.T

    z_tables = [out_table(slot, width_z, length, parts_y) for slot in range(len(OUT_SLOTS))]
    z_tables.append(out_table(0, width_z, length, parts_y))
    z_back = back_table(width_z, length, parts_y)

    back_lanes = up_to(len(BACK_SLOTS) * width_z, LANES)
    ky_all = signed(jnp.arange(ky_count, dtype=jnp.int32), ky_count).reshape(parts_x, 1, width_y)
    ky_rows = jnp.broadcast_to(ky_all, (parts_x, 2, width_y)).reshape(-1, 1)
    ky_rows = jnp.broadcast_to(ky_rows, (2 * ky_count, LANES))
    kz_in, kz_back = [], []
    for py in range(parts_y):
        modes, inside = lane_modes(0, width_z, LANES, py * width_z)
        kz_in.append(jnp.where(inside, modes, 0))
        total = jnp.zeros((back_lanes,), jnp.int32)
        for name in ("ax", "ay"):
            modes, inside = lane_modes(BACK_SLOTS.index(name), width_z, back_lanes, py * width_z)
            total = total + jnp.where(inside, modes, 0)
        kz_back.append(total.reshape(-1, LANES))
    kz_in = jnp.stack(kz_in).astype(F32)
    kz_back = jnp.stack(kz_back).astype(F32)

    def turn(weight):
        split = weight.reshape(hid, 3, PATCH, PATCH, PATCH)
        return split.transpose(0, 4, 1, 2, 3).reshape(hid, feat)

    w_in_f = turn(w_in)
    w_out_t = turn(w_out.T)
    bias = jnp.broadcast_to(b_in[:, None], (hid, 2 * LANES))
    weights = (w_in_f, w_in_f.T, w_out_t, bias)

    spectra = make_spectra(ky, kz_col, state, cotangent)
    spectra = spectra.reshape(width_y, -1, 2 * length)
    exchange = functools.partial(
        lax.all_to_all, axis_name=("px", "py"), split_axis=0, concat_axis=0, tiled=True
    )
    arrived = []
    for j in range(chunks):
        table = x_rows[:, j].reshape(parts * span * 2, 2 * length)
        arrived.append(exchange(along_x(table, spectra, parts, span)))
    grid_sizes = (parts_x, parts_y, width_y, width_z, length)
    tables = (t_y, t_yb, z_tables, z_back)
    returned = []
    grads = 0.0
    for recv in arrived:
        sent, gin, gout = physical(
            recv, ky_rows, kz_in, kz_back, tables, weights, grid_sizes, back_lanes
        )
        returned.append(exchange(sent))
        grads = grads + jnp.concatenate([gin, gout], axis=1)

    x_back = jnp.concatenate(
        [
            jnp.concatenate([cosine, -sine], axis=1),
            jnp.concatenate([sine, cosine], axis=1),
        ],
        axis=0,
    ).astype(BF16)
    state_grad = finish(ky, kz_col, x_back, cotangent, returned)

    grads = exchange(grads.reshape(parts, hid // parts, -1))
    grads = jnp.sum(grads, axis=0)
    own = hid // parts
    pad = up_to(feat + 1, 2 * LANES)

    def unturn(weight):
        split = weight.reshape(own, PATCH, 3, PATCH, PATCH)
        return split.transpose(0, 2, 3, 4, 1).reshape(own, feat)

    grad_in = unturn(grads[:, :feat])
    grad_bias = grads[:, feat][None, :]
    grad_out = FORCING * unturn(grads[:, pad:]).T
    return state_grad, grad_in, grad_out, grad_bias


def solution(mesh):
    return jax.shard_map(
        shards,
        mesh=mesh,
        in_specs=(
            P("rep", None, "px", "py", None),
            P("rep", None, "px", "py", None),
            P(),
            P(),
            P(),
        ),
        out_specs=(
            P("rep", None, "px", "py", None),
            P(("px", "py"), "rep"),
            P("rep", ("px", "py")),
            P("rep", ("px", "py")),
        ),
        check_vma=False,
    )
```

```python
import functools
import math

import jax
import jax.numpy as jnp
import numpy as np
from jax import lax
from jax.experimental import pallas as pl
from jax.experimental.pallas import tpu as pltpu
from jax.sharding import PartitionSpec as P


PATCH = 4
NU_DT = 5e-05
TIME_STEP = 0.01
FORCING = 20.0
LANES = 128
F32 = jnp.float32
BF16 = jnp.bfloat16

OUT_SLOTS = ("uy", "uz", "ux", "wy", "wz", "fx", "fy", "fz")
MAX_CHUNKS = 4
PAIRS = 2
HID_BLOCKS = 1
UNROLL = 4
BACK_SLOTS = ("ax", "az", "gy", "gz", "ay")


def up_to(value, step):
    return -(-value // step) * step


def angles(leading, trailing, length):
    product = np.asarray(leading)[:, None] * np.asarray(trailing)[None, :] % length
    phases = product.astype(np.float32) * np.float32(2.0 * math.pi / length)
    factor = np.float32(1.0 / math.sqrt(length))
    return np.cos(phases) * factor, np.sin(phases) * factor


def mode_ids(count, length):
    counter = np.arange(count)
    return np.where(counter < count // 2, counter, counter + length - count)


def box_order(length):
    counter = np.arange(length)
    boxes = length // PATCH
    return counter % boxes * PATCH + counter // boxes


def signed(counter, length):
    return jnp.where(counter < length // 2, counter, counter - length).astype(F32)


def dot(a, b):
    return lax.dot_general(a, b, (((1,), (0,)), ((), ())), preferred_element_type=F32)


def dot_nt(a, b):
    return lax.dot_general(a, b, (((1,), (1,)), ((), ())), preferred_element_type=F32)


def dot_tn(a, b):
    return lax.dot_general(a, b, (((0,), (0,)), ((), ())), preferred_element_type=F32)


def lane_modes(slot, width_z, lanes, first):
    local = np.arange(lanes) - slot * width_z
    inside = (local >= 0) & (local < width_z)
    return np.where(inside, local, 0) + first, inside


def vregs_of(slot, width_z):
    return list(range(slot * width_z // LANES, ((slot + 1) * width_z - 1) // LANES + 1))


def spectra_kernel(ky_ref, kz_ref, state_ref, cot_ref, out_ref, *, block, length):
    cutoff = float(length // 3)
    wave_z = kz_ref[...]
    counter = lax.broadcasted_iota(jnp.int32, wave_z.shape, 1)
    wave_x = jnp.where(counter < length // 2, counter, counter - length).astype(F32)
    plane = wave_x * wave_x + wave_z * wave_z
    inside = (jnp.abs(wave_x) <= cutoff) & (wave_z <= cutoff)
    weight = jnp.where(wave_z == 0.0, 1.0, 2.0).astype(F32)
    base = pl.program_id(0) * block

    def one(k, carry):
        wave_y = ky_ref[base + k]
        kept = jnp.where(inside & (jnp.abs(wave_y) <= cutoff), 1.0, 0.0).astype(F32)
        square = plane + wave_y * wave_y
        damped = jnp.exp(-NU_DT * square)
        scale = kept * weight
        push = kept * damped * TIME_STEP
        inverse = 1.0 / jnp.maximum(square, 1.0)
        u = [[scale * state_ref[c, r, k] for r in range(2)] for c in range(3)]
        for r in range(2):
            lanes = pl.ds(r * length, length)
            g = [push * cot_ref[c, r, k] for c in range(3)]
            along = (wave_x * g[0] + wave_y * g[1] + wave_z * g[2]) * inverse
            sign = -1.0 if r == 0 else 1.0
            q = 1 - r
            wy = sign * (wave_z * u[0][q] - wave_x * u[2][q])
            wz = sign * (wave_x * u[1][q] - wave_y * u[0][q])
            fx = g[0] - wave_x * along
            fy = g[1] - wave_y * along
            fz = g[2] - wave_z * along
            rows = (u[1][r], u[2][r], u[0][r], wy, wz, fx, fy, fz)
            for slot, value in enumerate(rows):
                out_ref[k, slot, :, lanes] = value.astype(BF16)
        return carry

    lax.fori_loop(0, block, one, 0)


def make_spectra(ky, kz_col, state, cotangent):
    _, _, width_y, width_z, length = state.shape
    block = 8
    slots = len(OUT_SLOTS)
    spec = pl.BlockSpec((3, 2, block, width_z, length), lambda i: (0, 0, i, 0, 0))
    return pl.pallas_call(
        functools.partial(spectra_kernel, block=block, length=length),
        grid=(width_y // block,),
        in_specs=[
            pl.BlockSpec(memory_space=pltpu.SMEM),
            pl.BlockSpec((width_z, length), lambda i: (0, 0)),
            spec,
            spec,
        ],
        out_specs=pl.BlockSpec((block, slots, width_z, 2 * length), lambda i: (i, 0, 0, 0)),
        out_shape=jax.ShapeDtypeStruct((width_y, slots, width_z, 2 * length), BF16),
        compiler_params=pltpu.CompilerParams(vmem_limit_bytes=56 * 2**20),
        name="spectra",
    )(ky, kz_col, state, cotangent)


def along_x_kernel(
    partner_ref, table_ref, spec_ref, *refs, first, chunks, block, width_y, span, parts
):
    out_refs, scratch = refs[:-1], refs[-1]
    step = pl.program_id(0)
    lanes = out_refs[0].shape[2]
    live = spec_ref.shape[1]
    pieces = [
        table_ref[partner_ref[k], first + j] for j in range(chunks) for k in range(parts)
    ]
    table = jnp.concatenate(pieces, axis=0)
    rows = table.shape[0]

    def one(k, carry):
        value = dot_nt(table, spec_ref[k])
        start = pl.multiple_of((step * block + k) * rows, 8)
        for v in range(lanes // LANES):
            if (v + 1) * LANES <= live:
                piece = value[:, v * LANES : (v + 1) * LANES]
                scratch[v, pl.ds(start, rows), :] = piece
            else:
                scratch[v, pl.ds(start, rows), :] = jnp.zeros((rows, LANES), F32)
                scratch[v, pl.ds(start, rows), pl.ds(0, live - v * LANES)] = value[:, v * LANES :]
        return carry

    lax.fori_loop(0, block, one, 0)

    @pl.when(step == pl.num_programs(0) - 1)
    def _():
        def move(x, carry):
            for target, out_ref in enumerate(out_refs):
                at = target * 2 * span + x
                for v in range(lanes // LANES):
                    sides = [
                        scratch[v, pl.ds(at + s * span, width_y, stride=rows), :] for s in range(2)
                    ]
                    block_rows = jnp.concatenate(sides, axis=0).astype(BF16)
                    out_ref[x, :, pl.ds(v * LANES, LANES)] = block_rows
            return carry

        lax.fori_loop(0, span, move, 0)


def along_x(partners, table, spectra, first, chunks):
    width_y, live, depth = spectra.shape
    parts = table.shape[0]
    span = table.shape[2] // 2
    rows = chunks * parts * 2 * span
    block = 8
    lanes = up_to(live, LANES)
    shape = (span, 2 * width_y, lanes)
    outs = pl.pallas_call(
        functools.partial(
            along_x_kernel,
            first=first,
            chunks=chunks,
            block=block,
            width_y=width_y,
            span=span,
            parts=parts,
        ),
        grid=(width_y // block,),
        in_specs=[
            pl.BlockSpec(memory_space=pltpu.SMEM),
            pl.BlockSpec(table.shape, lambda i: (0, 0, 0, 0)),
            pl.BlockSpec((block, live, depth), lambda i: (i, 0, 0)),
        ],
        out_specs=[pl.BlockSpec(shape, lambda i: (0, 0, 0))] * (parts * chunks),
        out_shape=[jax.ShapeDtypeStruct(shape, BF16)] * (parts * chunks),
        scratch_shapes=[pltpu.VMEM((lanes // LANES, width_y * rows, LANES), F32)],
        compiler_params=pltpu.CompilerParams(vmem_limit_bytes=58 * 2**20),
        cost_estimate=pl.CostEstimate(
            flops=2 * rows * live * depth * width_y * 2,
            bytes_accessed=2 * (width_y * live * depth + rows * width_y * lanes),
            transcendentals=0,
        ),
        name="along_x",
    )(partners, table, spectra)
    return [outs[j * parts : (j + 1) * parts] for j in range(chunks)]


def quads(low, high):
    upper = lax.broadcasted_iota(jnp.int32, low.shape, 1) < PATCH
    turned_high = pltpu.roll(high, PATCH, 1)
    turned_low = pltpu.roll(low, PATCH, 1)
    return jnp.where(upper, low, turned_high), jnp.where(upper, turned_low, high)


def halves(low, high):
    left = lax.broadcasted_iota(jnp.int32, low.shape, 1) < LANES // 2
    turned_high = pltpu.roll(high, LANES // 2, 1)
    turned_low = pltpu.roll(low, LANES // 2, 1)
    return jnp.where(left, low, turned_high), jnp.where(left, turned_low, high)


def physical_kernel(
    *refs,
    parts_x,
    parts_y,
    width_y,
    width_z,
    length,
    back_lanes,
):
    parts = parts_x * parts_y
    recv_refs, refs = refs[:parts], refs[parts:]
    physical_body(
        recv_refs, *refs, parts_x=parts_x, parts_y=parts_y, width_y=width_y,
        width_z=width_z, length=length, back_lanes=back_lanes,
    )


def physical_body(
    recv_refs,
    place_ref,
    ky_ref,
    kz_in_ref,
    kz_back_ref,
    ty_ref,
    tyb_ref,
    w_in_ref,
    w_in_t_ref,
    w_out_t_ref,
    bias_ref,
    *refs,
    parts_x,
    parts_y,
    width_y,
    width_z,
    length,
    back_lanes,
):
    z_refs = dict(zip(("uy", "uz", "ux", "wy", "wz", "fx", "fy", "fz", "wx"), refs[:9]))
    zb_ref = refs[9]
    parts = parts_x * parts_y
    out_refs, refs = refs[10 : 10 + parts], refs[10 + parts :]
    gin_ref, gout_ref = refs[:2]
    mid, vel, force, fields, fadj, back = refs[2:]
    rows = 2 * width_y
    in_lanes = recv_refs[0].shape[2]
    boxes = length // PATCH
    feats = 3 * PATCH * PATCH

    @pl.when(pl.program_id(0) == 0)
    def _():
        gin_ref[...] = jnp.zeros(gin_ref.shape, F32)
        gout_ref[...] = jnp.zeros(gout_ref.shape, F32)

    def section_y(dx, carry):
        for py in range(parts_y):
            whole = jnp.concatenate(
                [recv_refs[px * parts_y + py][dx] for px in range(parts_x)], axis=0
            )
            first = whole[:, :LANES].astype(F32)
            second = pltpu.roll(first, LANES - width_z, 1)
            mixed = ky_ref[...] * second - kz_in_ref[place_ref[1] ^ py] * first
            turned = []
            for px in range(parts_x):
                turned.append(-mixed[px * rows + width_y : (px + 1) * rows])
                turned.append(mixed[px * rows : px * rows + width_y])
            extra = jnp.concatenate(turned, axis=0).astype(BF16)
            mid[py, dx, :, pl.ds(0, in_lanes)] = dot(ty_ref[...], whole).astype(BF16)
            mid[py, dx, :, pl.ds(in_lanes, LANES)] = dot(ty_ref[...], extra).astype(BF16)
        return carry

    lax.fori_loop(0, PATCH, section_y, 0)

    def section_z(pair, carry):
        def field(name, dx):
            if name == "wx":
                vregs = [in_lanes // LANES]
            else:
                vregs = vregs_of(OUT_SLOTS.index(name), width_z)
            pieces = [
                mid[py, dx, pl.ds(t * length, length), pl.ds(v * LANES, LANES)]
                for py in range(parts_y)
                for t in range(2)
                for v in vregs
            ]
            table = [z_refs[name][place_ref[1] ^ py] for py in range(parts_y)]
            joined = jnp.concatenate(pieces, axis=1)
            return dot(joined, jnp.concatenate(table, axis=0)).astype(BF16)

        for kind, target in (("u", vel), ("f", force), ("w", None)):
            for slot, name in enumerate("xyz"):
                planes = []
                for i in range(2):
                    value = field(kind + name, 2 * pair + i)
                    fields["ufw".index(kind), slot, 2 * pair + i] = value
                    planes.append(value.astype(F32))
                if target is None:
                    continue
                rows_here = pl.ds(pl.multiple_of(slot * PATCH * PATCH + pair * 8, 8), 8)
                for half in range(length // LANES):
                    cut = slice(half * LANES, (half + 1) * LANES)
                    tiles = [value[:, cut].reshape(length // 8, 8, LANES) for value in planes]
                    for parity, value in enumerate(quads(*tiles)):
                        target[half, parity, :, rows_here, :] = value
        return carry

    lax.fori_loop(0, PATCH // 2, section_z, 0)

    def gather(source, at):
        per_dz = []
        for half in range(2):
            got = [
                halves(source[half, 0, at + p], source[half, 1, at + p])
                for p in range(PAIRS)
            ]
            for i in range(2):
                per_dz.append(jnp.concatenate([one[i] for one in got], axis=1))
        return jnp.concatenate(per_dz, axis=0).astype(BF16)

    hid = gin_ref.shape[0]
    unit = hid // HID_BLOCKS

    def closure(step, carry):
        at = step * PAIRS
        features = gather(vel, at)
        adjoints = gather(force, at)
        ones = jnp.ones((gin_ref.shape[1] - features.shape[0], features.shape[1]), BF16)
        extended = jnp.concatenate([features, ones], axis=0)
        pre_adjs = []
        for h in range(HID_BLOCKS):
            cut = pl.ds(h * unit, unit)
            bias = jnp.concatenate([bias_ref[cut, :]] * PAIRS, axis=1)
            pre = dot(w_in_ref[cut, :], features) + bias
            turned = jnp.tanh(0.5 * pre)
            sigma = 0.5 * turned + 0.5
            hidden = (pre * sigma).astype(BF16)
            hidden_adj = dot(w_out_t_ref[cut, :], adjoints)
            slope = FORCING * sigma + pre * ((0.5 * FORCING) * sigma * (1.0 - turned))
            pre_adj = (hidden_adj * slope).astype(BF16)
            gin_ref[cut, :] += dot_nt(pre_adj, extended)
            gout_ref[cut, :] += dot_nt(hidden, adjoints)
            pre_adjs.append(pre_adj)
        back_feat = dot(w_in_t_ref[...], jnp.concatenate(pre_adjs, axis=0))
        for half in range(2):
            low = back_feat[(2 * half) * feats : (2 * half + 1) * feats]
            high = back_feat[(2 * half + 1) * feats : (2 * half + 2) * feats]
            for p in range(PAIRS):
                cut = slice(p * LANES, (p + 1) * LANES)
                for parity, value in enumerate(halves(low[:, cut], high[:, cut])):
                    fadj[half, parity, at + p] = value
        return carry

    lax.fori_loop(0, boxes // (2 * PAIRS), closure, 0, unroll=UNROLL)

    back_vregs = back_lanes // LANES

    def section_back(pair, carry):
        adjoint = []
        for slot in range(3):
            rows_here = pl.ds(pl.multiple_of(slot * PATCH * PATCH + pair * 8, 8), 8)
            sides = [
                quads(fadj[half, 0, :, rows_here, :], fadj[half, 1, :, rows_here, :])
                for half in range(length // LANES)
            ]
            adjoint.append(
                [
                    jnp.concatenate([side[i].reshape(length, LANES) for side in sides], axis=1)
                    for i in range(2)
                ]
            )
        for i in range(2):
            one_plane(2 * pair + i, [value[i] for value in adjoint])
        return carry

    def one_plane(dx, adjoint):
        u, f, w = ([fields[k, c, dx].astype(F32) for c in range(3)] for k in range(3))
        named = {}
        for c, name in enumerate("xyz"):
            a, b = (c + 1) % 3, (c + 2) % 3
            turned = adjoint[c] + (w[a] * f[b] - w[b] * f[a])
            named["v" + name] = turned.astype(BF16)
            named["g" + name] = (f[a] * u[b] - f[b] * u[a]).astype(BF16)
        at = 0
        for group, names in enumerate(back_groups(width_z)):
            joined = jnp.concatenate([named[name] for name in names], axis=1)
            depth = joined.shape[1]
            for py in range(parts_y):
                table = zb_ref[place_ref[1] ^ py, pl.ds(at, depth), :]
                value = dot(joined, table).astype(BF16)
                for r in range(2):
                    piece = value[:, r * LANES : (r + 1) * LANES]
                    back[py, pl.ds(r * length, length), pl.ds(group * LANES, LANES)] = piece
            at += depth
        for py in range(parts_y):
            table = [tyb_ref[place_ref[0] ^ px] for px in range(parts_x)]
            value = dot(jnp.concatenate(table, axis=0), back[py])
            by_y = ky_ref[...] * value[:, back_lanes : back_lanes + LANES]
            by_z = value[:, back_lanes + LANES :]
            extra = []
            for v in range(back_vregs):
                here = kz_back_ref[place_ref[1] ^ py, v] * by_z
                if v == 0:
                    here = here + by_y
                extra.append(here)
            extra = jnp.concatenate(extra, axis=1)
            for px in range(parts_x):
                re = slice(px * rows, px * rows + width_y)
                im = slice(px * rows + width_y, (px + 1) * rows)
                total = jnp.concatenate(
                    [value[re, :back_lanes] - extra[im], value[im, :back_lanes] + extra[re]], axis=0
                )
                out_refs[px * parts_y + py][dx] = total.astype(BF16)

    lax.fori_loop(0, PATCH // 2, section_back, 0)


def back_groups(width_z):
    names = [{"a": "v", "g": "g"}[slot[0]] + slot[1] for slot in BACK_SLOTS]
    lanes = up_to(len(BACK_SLOTS) * width_z, LANES)
    groups = []
    for v in range(lanes // LANES):
        groups.append([n for slot, n in enumerate(names) if v in vregs_of(slot, width_z)])
    groups.append(["gz", "gx"])
    groups.append(["gy", "gx"])
    return groups


def back_table(width_z, length, parts_y):
    names = [{"a": "v", "g": "g"}[slot[0]] + slot[1] for slot in BACK_SLOTS]
    lanes = up_to(len(BACK_SLOTS) * width_z, LANES)
    groups = back_groups(width_z)
    order = box_order(length)

    def piece(slot, vreg, py, sign):
        modes, inside = lane_modes(slot, width_z, lanes, py * width_z)
        cut = slice(vreg * LANES, (vreg + 1) * LANES)
        cosine, sine = angles(order, modes[cut], length)
        keep = sign * inside[cut].astype(np.float32)[None, :]
        return np.concatenate([cosine * keep, -sine * keep], axis=1)

    ky_slots = {"gz": (BACK_SLOTS.index("ax"), 1.0), "gx": (BACK_SLOTS.index("az"), -1.0)}
    kz_slots = {"gy": (BACK_SLOTS.index("ax"), -1.0), "gx": (BACK_SLOTS.index("ay"), 1.0)}
    tables = []
    for py in range(parts_y):
        rows = []
        for v, group in enumerate(groups[:-2]):
            rows += [piece(names.index(n), v, py, 1.0) for n in group]
        for which, group in ((ky_slots, groups[-2]), (kz_slots, groups[-1])):
            for n in group:
                slot, sign = which[n]
                rows.append(sum(piece(slot, v, py, sign) for v in vregs_of(slot, width_z)))
        tables.append(np.concatenate(rows, axis=0))
    return jnp.asarray(np.stack(tables), BF16)


def out_table(slot, width_z, length, parts_y):
    lanes = (vregs_of(slot, width_z)[-1] + 1) * LANES
    order = box_order(length)
    tables = []
    for py in range(parts_y):
        modes, inside = lane_modes(slot, width_z, lanes, py * width_z)
        cosine, sine = angles(modes, order, length)
        keep = inside.astype(np.float32)[:, None]
        rows = []
        for value in (cosine, -sine):
            for v in vregs_of(slot, width_z):
                rows.append((value * keep)[v * LANES : (v + 1) * LANES])
        tables.append(np.concatenate(rows, axis=0))
    return jnp.asarray(np.stack(tables), BF16)


def physical(recv, place, ky_rows, kz_in, kz_back, tables, weights, grid_sizes, back_lanes):
    parts_x, parts_y, width_y, width_z, length = grid_sizes
    parts = parts_x * parts_y
    span, rows, in_lanes = recv[0].shape
    hid = weights[0].shape[0]
    feat = weights[0].shape[1]
    t_y, t_yb, z_tables, z_back = tables

    def whole(array):
        return pl.BlockSpec(array.shape, lambda i: (0,) * array.ndim)

    small = [ky_rows, kz_in, kz_back, t_y, t_yb, *weights, *z_tables, z_back]
    feat_pad = up_to(feat + 1, 2 * LANES)
    boxed = (length // LANES, 2, length // (2 * PATCH), 3 * PATCH * PATCH, LANES)
    flops = 2 * span * parts_y * (2 * length) * (parts_x * rows) * (in_lanes + LANES)
    flops += 2 * 5 * hid * feat * (span * length * length // PATCH**3)
    flops += 2 * span * length * length * length * (9 * 2 + 20)
    return pl.pallas_call(
        functools.partial(
            physical_kernel,
            parts_x=parts_x,
            parts_y=parts_y,
            width_y=width_y,
            width_z=width_z,
            length=length,
            back_lanes=back_lanes,
        ),
        grid=(span // PATCH,),
        in_specs=[pl.BlockSpec((PATCH, rows, in_lanes), lambda i: (i, 0, 0))] * parts
        + [pl.BlockSpec(memory_space=pltpu.SMEM)]
        + [whole(a) for a in small],
        out_specs=[pl.BlockSpec((PATCH, rows, back_lanes), lambda i: (i, 0, 0))] * parts
        + [
            pl.BlockSpec((hid, feat_pad), lambda i: (0, 0)),
            pl.BlockSpec((hid, feat), lambda i: (0, 0)),
        ],
        out_shape=[jax.ShapeDtypeStruct((span, rows, back_lanes), BF16)] * parts
        + [
            jax.ShapeDtypeStruct((hid, feat_pad), F32),
            jax.ShapeDtypeStruct((hid, feat), F32),
        ],
        scratch_shapes=[
            pltpu.VMEM((parts_y, PATCH, 2 * length, in_lanes + LANES), BF16),
            pltpu.VMEM(boxed, F32),
            pltpu.VMEM(boxed, F32),
            pltpu.VMEM((3, 3, PATCH, length, length), BF16),
            pltpu.VMEM(boxed, F32),
            pltpu.VMEM((parts_y, 2 * length, back_lanes + 2 * LANES), BF16),
        ],
        compiler_params=pltpu.CompilerParams(vmem_limit_bytes=58 * 2**20),
        cost_estimate=pl.CostEstimate(
            flops=flops, bytes_accessed=4 * parts * recv[0].size, transcendentals=0
        ),
        name="physical",
    )(*recv, place, *small)


def final_kernel(
    partner_ref, ky_ref, kz_ref, table_ref, cot_ref, *refs, steps_in, block, width_y, width_z, length
):
    out_ref, scratch, turned = refs[-3:]
    recv_refs = refs[:-3]
    parts = partner_ref.shape[0]
    step = pl.program_id(0)
    rows = 2 * width_y
    lanes = recv_refs[0].shape[2]

    @pl.when(step < steps_in)
    def _():
        for j, recv_ref in enumerate(recv_refs):
            source = partner_ref[j % parts]
            x = source * (length // parts) + (j // parts) * steps_in + step
            at = pl.multiple_of(x * rows, 8)
            value = recv_ref[0].astype(F32)
            for v in range(lanes // LANES):
                scratch[v, pl.ds(at, rows), :] = value[:, v * LANES : (v + 1) * LANES]

    @pl.when(step >= steps_in)
    def _():
        cutoff = float(length // 3)
        wave_z = kz_ref[...]
        counter = lax.broadcasted_iota(jnp.int32, wave_z.shape, 1)
        wave_x = jnp.where(counter < length // 2, counter, counter - length).astype(F32)
        plane = wave_x * wave_x + wave_z * wave_z
        inside = (jnp.abs(wave_x) <= cutoff) & (wave_z <= cutoff)
        weight = jnp.where(wave_z == 0.0, 1.0, 2.0).astype(F32)

        def one(k, carry):
            ky = (step - steps_in) * block + k
            pieces = []
            for v in range(lanes // LANES):
                parts_s = [
                    scratch[v, pl.ds(ky + s * width_y, length, stride=rows), :] for s in range(2)
                ]
                pieces.append(jnp.concatenate(parts_s, axis=0))
            gathered = jnp.concatenate(pieces, axis=1).astype(BF16)
            turned[...] = dot_tn(gathered, table_ref[...])
            wave_y = ky_ref[ky]
            kept = jnp.where(inside & (jnp.abs(wave_y) <= cutoff), 1.0, 0.0).astype(F32)
            damped = jnp.exp(-NU_DT * (plane + wave_y * wave_y))
            scale = kept * weight

            def part(name, t):
                at = BACK_SLOTS.index(name) * width_z
                return turned[pl.ds(at, width_z), pl.ds(t * length, length)]

            for t in range(2):
                sign = -1.0 if t == 0 else 1.0
                ax = part("ax", t)
                ay = part("ay", t) - sign * wave_x * part("gz", 1 - t)
                az = part("az", t) + sign * wave_x * part("gy", 1 - t)
                for c, value in enumerate((ax, ay, az)):
                    out_ref[c, t, k] = damped * cot_ref[c, t, k] + scale * value
            return carry

        lax.fori_loop(0, block, one, 0)


def finish(partners, ky, kz_col, table, cotangent, received):
    _, _, width_y, width_z, length = cotangent.shape
    span, rows, lanes = received[0].shape
    block = 8
    steps_in = span
    steps = steps_in + width_y // block
    spec = pl.BlockSpec(
        (3, 2, block, width_z, length), lambda i: (0, 0, jnp.maximum(i - steps_in, 0), 0, 0)
    )
    recv_spec = pl.BlockSpec((1, rows, lanes), lambda i: (jnp.minimum(i, steps_in - 1), 0, 0))
    return pl.pallas_call(
        functools.partial(
            final_kernel,
            steps_in=steps_in,
            block=block,
            width_y=width_y,
            width_z=width_z,
            length=length,
        ),
        grid=(steps,),
        in_specs=[
            pl.BlockSpec(memory_space=pltpu.SMEM),
            pl.BlockSpec(memory_space=pltpu.SMEM),
            pl.BlockSpec((width_z, length), lambda i: (0, 0)),
            pl.BlockSpec(table.shape, lambda i: (0, 0)),
            spec,
        ]
        + [recv_spec] * len(received),
        out_specs=spec,
        out_shape=jax.ShapeDtypeStruct(cotangent.shape, F32),
        scratch_shapes=[
            pltpu.VMEM((lanes // LANES, length * rows, LANES), F32),
            pltpu.VMEM((lanes, 2 * length), F32),
        ],
        compiler_params=pltpu.CompilerParams(vmem_limit_bytes=60 * 2**20),
        name="finish",
    )(partners, ky, kz_col, table, cotangent, *received)


def shards(state, cotangent, w_in, b_in, w_out):
    width_y, width_z, length = state.shape[2:]
    parts_x = lax.axis_size("px")
    parts_y = lax.axis_size("py")
    parts = parts_x * parts_y
    slab = length // parts
    chunks = MAX_CHUNKS
    while chunks > 1 and slab % (chunks * PATCH) != 0:
        chunks //= 2
    span = slab // chunks
    ky_count = width_y * parts_x
    hid, feat = w_in.shape

    own_x = lax.axis_index("px")
    own_y = lax.axis_index("py")
    own = own_x * parts_y + own_y
    partners = own ^ jnp.arange(parts, dtype=jnp.int32)
    partners_x = own_x ^ jnp.arange(parts_x, dtype=jnp.int32)
    local_y = jnp.arange(width_y, dtype=jnp.int32)
    ky_ids = own_x * width_y + local_y
    kz_ids = own_y * width_z + jnp.arange(width_z, dtype=jnp.int32)
    ky = signed(ky_ids, ky_count)
    kz_col = jnp.broadcast_to(kz_ids.astype(F32)[:, None], (width_z, length))

    everything = np.arange(length)
    cosine, sine = angles(everything, everything, length)
    both = np.stack(
        [np.concatenate([cosine, -sine], axis=1), np.concatenate([sine, cosine], axis=1)]
    )
    x_back = jnp.asarray(both.reshape(2 * length, 2 * length), BF16)
    x_rows = both.reshape(2, parts, chunks, span, 2 * length).transpose(1, 2, 0, 3, 4)
    x_rows = jnp.asarray(x_rows.reshape(parts, chunks, 2 * span, 2 * length), BF16)

    ky_modes = mode_ids(ky_count, length)
    cosine, sine = angles(everything, ky_modes, length)
    cosine = cosine.reshape(length, parts_x, width_y)
    sine = sine.reshape(length, parts_x, width_y)
    t_y = np.stack(
        [np.concatenate([cosine, -sine], axis=2), np.concatenate([sine, cosine], axis=2)]
    )
    t_yb = jnp.asarray(t_y.reshape(2 * length, parts_x, -1).transpose(1, 2, 0), BF16)
    t_y = jnp.asarray(t_y.reshape(2 * length, parts_x, -1), BF16)
    t_y = jnp.take(t_y, partners_x, axis=1).reshape(2 * length, -1)

    z_tables = [out_table(slot, width_z, length, parts_y) for slot in range(len(OUT_SLOTS))]
    z_tables.append(z_tables[0])
    z_back = back_table(width_z, length, parts_y)

    back_lanes = up_to(len(BACK_SLOTS) * width_z, LANES)
    ky_order = (partners_x[:, None] * width_y + local_y[None, :]).astype(jnp.int32)
    ky_rows = signed(ky_order, ky_count).reshape(parts_x, 1, width_y, 1)
    ky_rows = jnp.broadcast_to(ky_rows, (parts_x, 2, width_y, LANES)).reshape(-1, LANES)
    kz_in, kz_back = [], []
    for py in range(parts_y):
        modes, inside = lane_modes(0, width_z, LANES, py * width_z)
        kz_in.append(np.where(inside, modes, 0)[None, :])
        total = np.zeros((back_lanes,))
        for name in ("ax", "ay"):
            slot = BACK_SLOTS.index(name)
            modes, inside = lane_modes(slot, width_z, back_lanes, py * width_z)
            total = total + np.where(inside, modes, 0)
        kz_back.append(total.reshape(-1, 1, LANES))
    kz_in = jnp.asarray(np.stack(kz_in), F32)
    kz_back = jnp.asarray(np.stack(kz_back), F32)

    units = hid // parts

    def turn(weight):
        split = weight.reshape(parts, units, 3, PATCH, PATCH, PATCH)[partners]
        return split.transpose(0, 1, 5, 2, 3, 4).reshape(hid, feat)

    w_in_f = turn(w_in)
    w_out_t = turn(w_out.T)
    bias = b_in.reshape(parts, units)[partners].reshape(hid, 1)
    bias = jnp.broadcast_to(bias, (hid, LANES))
    weights = (w_in_f, w_in_f.T, w_out_t, bias)

    def exchange(arrays):
        moved = [arrays[0]]
        for k in range(1, parts):
            pairs = [(i, i ^ k) for i in range(parts)]
            moved.append(lax.ppermute(arrays[k], ("px", "py"), pairs))
        return moved

    spectra = make_spectra(ky, kz_col, state, cotangent)
    spectra = spectra.reshape(width_y, -1, 2 * length)
    arrived = []
    groups = ((0, 1), (1, 1), (2, 2)) if chunks == 4 else tuple((j, 1) for j in range(chunks))
    for first, count in groups:
        outs = along_x(partners, x_rows, spectra, first, count)
        for sent in outs:
            arrived.append(exchange(sent))
    place = jnp.stack([own_x, own_y]).astype(jnp.int32)
    grid_sizes = (parts_x, parts_y, width_y, width_z, length)
    tables = (t_y, t_yb, z_tables, z_back)
    returned = []
    grads = 0.0
    for recv in arrived:
        *sent, gin, gout = physical(
            recv, place, ky_rows, kz_in, kz_back, tables, weights, grid_sizes, back_lanes
        )
        returned.append(exchange(sent))
        grads = grads + jnp.concatenate([gin, gout], axis=1)
    grads = sum(exchange([grads[k * units : (k + 1) * units] for k in range(parts)]))

    received = [array for chunk in returned for array in chunk]
    state_grad = finish(partners, ky, kz_col, x_back, cotangent, received)

    pad = up_to(feat + 1, 2 * LANES)

    def unturn(weight):
        split = weight.reshape(units, PATCH, 3, PATCH, PATCH)
        return split.transpose(0, 2, 3, 4, 1).reshape(units, feat)

    grad_in = unturn(grads[:, :feat])
    grad_bias = grads[:, feat][None, :]
    grad_out = FORCING * unturn(grads[:, pad:]).T
    return state_grad, grad_in, grad_out, grad_bias


def solution(mesh):
    return jax.shard_map(
        shards,
        mesh=mesh,
        in_specs=(
            P("rep", None, "px", "py", None),
            P("rep", None, "px", "py", None),
            P(),
            P(),
            P(),
        ),
        out_specs=(
            P("rep", None, "px", "py", None),
            P(("px", "py"), "rep"),
            P("rep", ("px", "py")),
            P("rep", ("px", "py")),
        ),
        check_vma=False,
    )
```

```python
import functools
import math

import jax
import jax.numpy as jnp
import numpy as np
from jax import lax
from jax.experimental import pallas as pl
from jax.experimental.pallas import tpu as pltpu
from jax.sharding import PartitionSpec as P


PATCH = 4
NU_DT = 5e-05
TIME_STEP = 0.01
FORCING = 20.0
LANES = 128
F32 = jnp.float32
BF16 = jnp.bfloat16

OUT_SLOTS = ("uy", "uz", "ux", "wy", "wz", "fx", "fy", "fz")
MAX_CHUNKS = 4
PAIRS = 2
WAVE_UNROLL = 4
MOVE_UNROLL = 1
LAST_UNROLL = 2
SPEC_UNROLL = 1
PLANE_UNROLL = 2
HID_BLOCKS = 1
UNROLL = 4
BACK_SLOTS = ("ax", "az", "gy", "gz", "ay")


def up_to(value, step):
    return -(-value // step) * step


def angles(leading, trailing, length):
    product = np.asarray(leading)[:, None] * np.asarray(trailing)[None, :] % length
    phases = product.astype(np.float32) * np.float32(2.0 * math.pi / length)
    factor = np.float32(1.0 / math.sqrt(length))
    return np.cos(phases) * factor, np.sin(phases) * factor


def mode_ids(count, length):
    counter = np.arange(count)
    return np.where(counter < count // 2, counter, counter + length - count)


def box_order(length):
    counter = np.arange(length)
    boxes = length // PATCH
    return counter % boxes * PATCH + counter // boxes


def signed(counter, length):
    return jnp.where(counter < length // 2, counter, counter - length).astype(F32)


def dot(a, b):
    return lax.dot_general(a, b, (((1,), (0,)), ((), ())), preferred_element_type=F32)


def dot_nt(a, b):
    return lax.dot_general(a, b, (((1,), (1,)), ((), ())), preferred_element_type=F32)


def dot_tn(a, b):
    return lax.dot_general(a, b, (((0,), (0,)), ((), ())), preferred_element_type=F32)


def lane_modes(slot, width_z, lanes, first):
    local = np.arange(lanes) - slot * width_z
    inside = (local >= 0) & (local < width_z)
    return np.where(inside, local, 0) + first, inside


def vregs_of(slot, width_z):
    return list(range(slot * width_z // LANES, ((slot + 1) * width_z - 1) // LANES + 1))


def spectra_kernel(ky_ref, kz_ref, state_ref, cot_ref, out_ref, *, block, length):
    cutoff = float(length // 3)
    wave_z = kz_ref[...]
    counter = lax.broadcasted_iota(jnp.int32, wave_z.shape, 1)
    wave_x = jnp.where(counter < length // 2, counter, counter - length).astype(F32)
    plane = wave_x * wave_x + wave_z * wave_z
    inside = (jnp.abs(wave_x) <= cutoff) & (wave_z <= cutoff)
    weight = jnp.where(wave_z == 0.0, 1.0, 2.0).astype(F32)
    base = pl.program_id(0) * block

    def one(k, carry):
        wave_y = ky_ref[base + k]
        kept = jnp.where(inside & (jnp.abs(wave_y) <= cutoff), 1.0, 0.0).astype(F32)
        square = plane + wave_y * wave_y
        damped = jnp.exp(-NU_DT * square)
        scale = kept * weight
        push = kept * damped * TIME_STEP
        inverse = 1.0 / jnp.maximum(square, 1.0)
        u = [[scale * state_ref[c, r, k] for r in range(2)] for c in range(3)]
        for r in range(2):
            lanes = pl.ds(r * length, length)
            g = [push * cot_ref[c, r, k] for c in range(3)]
            along = (wave_x * g[0] + wave_y * g[1] + wave_z * g[2]) * inverse
            sign = -1.0 if r == 0 else 1.0
            q = 1 - r
            wy = sign * (wave_z * u[0][q] - wave_x * u[2][q])
            wz = sign * (wave_x * u[1][q] - wave_y * u[0][q])
            fx = g[0] - wave_x * along
            fy = g[1] - wave_y * along
            fz = g[2] - wave_z * along
            rows = (u[1][r], u[2][r], u[0][r], wy, wz, fx, fy, fz)
            for slot, value in enumerate(rows):
                out_ref[k, slot, :, lanes] = value.astype(BF16)
        return carry

    lax.fori_loop(0, block, one, 0, unroll=SPEC_UNROLL)


def make_spectra(ky, kz_col, state, cotangent):
    _, _, width_y, width_z, length = state.shape
    block = 8
    slots = len(OUT_SLOTS)
    spec = pl.BlockSpec((3, 2, block, width_z, length), lambda i: (0, 0, i, 0, 0))
    return pl.pallas_call(
        functools.partial(spectra_kernel, block=block, length=length),
        grid=(width_y // block,),
        in_specs=[
            pl.BlockSpec(memory_space=pltpu.SMEM),
            pl.BlockSpec((width_z, length), lambda i: (0, 0)),
            spec,
            spec,
        ],
        out_specs=pl.BlockSpec((block, slots, width_z, 2 * length), lambda i: (i, 0, 0, 0)),
        out_shape=jax.ShapeDtypeStruct((width_y, slots, width_z, 2 * length), BF16),
        compiler_params=pltpu.CompilerParams(vmem_limit_bytes=56 * 2**20),
        name="spectra",
    )(ky, kz_col, state, cotangent)


def along_x_kernel(
    partner_ref, table_ref, spec_ref, *refs, first, chunks, block, width_y, span, parts
):
    out_refs, scratch = refs[:-1], refs[-1]
    step = pl.program_id(0)
    lanes = out_refs[0].shape[2]
    live = spec_ref.shape[1]
    pieces = [
        table_ref[partner_ref[k], first + j] for j in range(chunks) for k in range(parts)
    ]
    table = jnp.concatenate(pieces, axis=0)
    rows = table.shape[0]

    def one(k, carry):
        value = dot_nt(table, spec_ref[k])
        start = pl.multiple_of((step * block + k) * rows, 8)
        for v in range(lanes // LANES):
            if (v + 1) * LANES <= live:
                piece = value[:, v * LANES : (v + 1) * LANES]
                scratch[v, pl.ds(start, rows), :] = piece
            else:
                scratch[v, pl.ds(start, rows), :] = jnp.zeros((rows, LANES), F32)
                scratch[v, pl.ds(start, rows), pl.ds(0, live - v * LANES)] = value[:, v * LANES :]
        return carry

    lax.fori_loop(0, block, one, 0, unroll=WAVE_UNROLL)

    @pl.when(step == pl.num_programs(0) - 1)
    def _():
        def move(x, carry):
            for target, out_ref in enumerate(out_refs):
                at = target * 2 * span + x
                for v in range(lanes // LANES):
                    sides = [
                        scratch[v, pl.ds(at + s * span, width_y, stride=rows), :] for s in range(2)
                    ]
                    block_rows = jnp.concatenate(sides, axis=0).astype(BF16)
                    out_ref[x, :, pl.ds(v * LANES, LANES)] = block_rows
            return carry

        lax.fori_loop(0, span, move, 0, unroll=MOVE_UNROLL)


def along_x(partners, table, spectra, first, chunks):
    width_y, live, depth = spectra.shape
    parts = table.shape[0]
    span = table.shape[2] // 2
    rows = chunks * parts * 2 * span
    block = 8
    lanes = up_to(live, LANES)
    shape = (span, 2 * width_y, lanes)
    outs = pl.pallas_call(
        functools.partial(
            along_x_kernel,
            first=first,
            chunks=chunks,
            block=block,
            width_y=width_y,
            span=span,
            parts=parts,
        ),
        grid=(width_y // block,),
        in_specs=[
            pl.BlockSpec(memory_space=pltpu.SMEM),
            pl.BlockSpec(table.shape, lambda i: (0, 0, 0, 0)),
            pl.BlockSpec((block, live, depth), lambda i: (i, 0, 0)),
        ],
        out_specs=[pl.BlockSpec(shape, lambda i: (0, 0, 0))] * (parts * chunks),
        out_shape=[jax.ShapeDtypeStruct(shape, BF16)] * (parts * chunks),
        scratch_shapes=[pltpu.VMEM((lanes // LANES, width_y * rows, LANES), F32)],
        compiler_params=pltpu.CompilerParams(vmem_limit_bytes=58 * 2**20),
        cost_estimate=pl.CostEstimate(
            flops=2 * rows * live * depth * width_y * 2,
            bytes_accessed=2 * (width_y * live * depth + rows * width_y * lanes),
            transcendentals=0,
        ),
        name="along_x",
    )(partners, table, spectra)
    return [outs[j * parts : (j + 1) * parts] for j in range(chunks)]


def quads(low, high):
    upper = lax.broadcasted_iota(jnp.int32, low.shape, 1) < PATCH
    turned_high = pltpu.roll(high, PATCH, 1)
    turned_low = pltpu.roll(low, PATCH, 1)
    return jnp.where(upper, low, turned_high), jnp.where(upper, turned_low, high)


def halves(low, high):
    left = lax.broadcasted_iota(jnp.int32, low.shape, 1) < LANES // 2
    turned_high = pltpu.roll(high, LANES // 2, 1)
    turned_low = pltpu.roll(low, LANES // 2, 1)
    return jnp.where(left, low, turned_high), jnp.where(left, turned_low, high)


def physical_kernel(
    *refs,
    parts_x,
    parts_y,
    width_y,
    width_z,
    length,
    back_lanes,
):
    parts = parts_x * parts_y
    recv_refs, refs = refs[:parts], refs[parts:]
    physical_body(
        recv_refs, *refs, parts_x=parts_x, parts_y=parts_y, width_y=width_y,
        width_z=width_z, length=length, back_lanes=back_lanes,
    )


def physical_body(
    recv_refs,
    place_ref,
    ky_ref,
    kz_in_ref,
    kz_back_ref,
    ty_ref,
    tyb_ref,
    w_in_ref,
    w_in_t_ref,
    w_out_t_ref,
    bias_ref,
    *refs,
    parts_x,
    parts_y,
    width_y,
    width_z,
    length,
    back_lanes,
):
    z_refs = dict(zip(("uy", "uz", "ux", "wy", "wz", "fx", "fy", "fz", "wx"), refs[:9]))
    zb_ref = refs[9]
    parts = parts_x * parts_y
    out_refs, refs = refs[10 : 10 + parts], refs[10 + parts :]
    gin_ref, gout_ref = refs[:2]
    mid, vel, force, fields, fadj, back = refs[2:]
    rows = 2 * width_y
    in_lanes = recv_refs[0].shape[2]
    boxes = length // PATCH
    feats = 3 * PATCH * PATCH

    @pl.when(pl.program_id(0) == 0)
    def _():
        gin_ref[...] = jnp.zeros(gin_ref.shape, F32)
        gout_ref[...] = jnp.zeros(gout_ref.shape, F32)

    def section_y(dx, carry):
        for py in range(parts_y):
            whole = jnp.concatenate(
                [recv_refs[px * parts_y + py][dx] for px in range(parts_x)], axis=0
            )
            first = whole[:, :LANES].astype(F32)
            second = pltpu.roll(first, LANES - width_z, 1)
            mixed = ky_ref[...] * second - kz_in_ref[place_ref[1] ^ py] * first
            turned = []
            for px in range(parts_x):
                turned.append(-mixed[px * rows + width_y : (px + 1) * rows])
                turned.append(mixed[px * rows : px * rows + width_y])
            extra = jnp.concatenate(turned, axis=0).astype(BF16)
            mid[py, dx, :, pl.ds(0, in_lanes)] = dot(ty_ref[...], whole).astype(BF16)
            mid[py, dx, :, pl.ds(in_lanes, LANES)] = dot(ty_ref[...], extra).astype(BF16)
        return carry

    lax.fori_loop(0, PATCH, section_y, 0, unroll=PLANE_UNROLL)

    def section_z(pair, carry):
        def field(name, dx):
            if name == "wx":
                vregs = [in_lanes // LANES]
            else:
                vregs = vregs_of(OUT_SLOTS.index(name), width_z)
            pieces = [
                mid[py, dx, pl.ds(t * length, length), pl.ds(v * LANES, LANES)]
                for py in range(parts_y)
                for t in range(2)
                for v in vregs
            ]
            table = [z_refs[name][place_ref[1] ^ py] for py in range(parts_y)]
            joined = jnp.concatenate(pieces, axis=1)
            return dot(joined, jnp.concatenate(table, axis=0)).astype(BF16)

        for kind, target in (("u", vel), ("f", force), ("w", None)):
            for slot, name in enumerate("xyz"):
                planes = []
                for i in range(2):
                    value = field(kind + name, 2 * pair + i)
                    fields["ufw".index(kind), slot, 2 * pair + i] = value
                    planes.append(value.astype(F32))
                if target is None:
                    continue
                rows_here = pl.ds(pl.multiple_of(slot * PATCH * PATCH + pair * 8, 8), 8)
                for half in range(length // LANES):
                    cut = slice(half * LANES, (half + 1) * LANES)
                    tiles = [value[:, cut].reshape(length // 8, 8, LANES) for value in planes]
                    for parity, value in enumerate(quads(*tiles)):
                        target[half, parity, :, rows_here, :] = value
        return carry

    lax.fori_loop(0, PATCH // 2, section_z, 0, unroll=PLANE_UNROLL)

    def gather(source, at):
        per_dz = []
        for half in range(2):
            got = [
                halves(source[half, 0, at + p], source[half, 1, at + p])
                for p in range(PAIRS)
            ]
            for i in range(2):
                per_dz.append(jnp.concatenate([one[i] for one in got], axis=1))
        return jnp.concatenate(per_dz, axis=0).astype(BF16)

    hid = gin_ref.shape[0]
    unit = hid // HID_BLOCKS

    def closure(step, carry):
        at = step * PAIRS
        features = gather(vel, at)
        adjoints = gather(force, at)
        ones = jnp.ones((gin_ref.shape[1] - features.shape[0], features.shape[1]), BF16)
        extended = jnp.concatenate([features, ones], axis=0)
        pre_adjs = []
        for h in range(HID_BLOCKS):
            cut = pl.ds(h * unit, unit)
            bias = jnp.concatenate([bias_ref[cut, :]] * PAIRS, axis=1)
            pre = dot(w_in_ref[cut, :], features) + bias
            turned = jnp.tanh(0.5 * pre)
            sigma = 0.5 * turned + 0.5
            hidden = (pre * sigma).astype(BF16)
            hidden_adj = dot(w_out_t_ref[cut, :], adjoints)
            slope = FORCING * sigma + pre * ((0.5 * FORCING) * sigma * (1.0 - turned))
            pre_adj = (hidden_adj * slope).astype(BF16)
            gin_ref[cut, :] += dot_nt(pre_adj, extended)
            gout_ref[cut, :] += dot_nt(hidden, adjoints)
            pre_adjs.append(pre_adj)
        back_feat = dot(w_in_t_ref[...], jnp.concatenate(pre_adjs, axis=0))
        for half in range(2):
            low = back_feat[(2 * half) * feats : (2 * half + 1) * feats]
            high = back_feat[(2 * half + 1) * feats : (2 * half + 2) * feats]
            for p in range(PAIRS):
                cut = slice(p * LANES, (p + 1) * LANES)
                for parity, value in enumerate(halves(low[:, cut], high[:, cut])):
                    fadj[half, parity, at + p] = value
        return carry

    lax.fori_loop(0, boxes // (2 * PAIRS), closure, 0, unroll=UNROLL)

    back_vregs = back_lanes // LANES

    def section_back(pair, carry):
        adjoint = []
        for slot in range(3):
            rows_here = pl.ds(pl.multiple_of(slot * PATCH * PATCH + pair * 8, 8), 8)
            sides = [
                quads(fadj[half, 0, :, rows_here, :], fadj[half, 1, :, rows_here, :])
                for half in range(length // LANES)
            ]
            adjoint.append(
                [
                    jnp.concatenate([side[i].reshape(length, LANES) for side in sides], axis=1)
                    for i in range(2)
                ]
            )
        for i in range(2):
            one_plane(2 * pair + i, [value[i] for value in adjoint])
        return carry

    def one_plane(dx, adjoint):
        u, f, w = ([fields[k, c, dx].astype(F32) for c in range(3)] for k in range(3))
        named = {}
        for c, name in enumerate("xyz"):
            a, b = (c + 1) % 3, (c + 2) % 3
            turned = adjoint[c] + (w[a] * f[b] - w[b] * f[a])
            named["v" + name] = turned.astype(BF16)
            named["g" + name] = (f[a] * u[b] - f[b] * u[a]).astype(BF16)
        at = 0
        for group, names in enumerate(back_groups(width_z)):
            joined = jnp.concatenate([named[name] for name in names], axis=1)
            depth = joined.shape[1]
            for py in range(parts_y):
                table = zb_ref[place_ref[1] ^ py, pl.ds(at, depth), :]
                value = dot(joined, table).astype(BF16)
                for r in range(2):
                    piece = value[:, r * LANES : (r + 1) * LANES]
                    back[py, pl.ds(r * length, length), pl.ds(group * LANES, LANES)] = piece
            at += depth
        for py in range(parts_y):
            table = [tyb_ref[place_ref[0] ^ px] for px in range(parts_x)]
            value = dot(jnp.concatenate(table, axis=0), back[py])
            by_y = ky_ref[...] * value[:, back_lanes : back_lanes + LANES]
            by_z = value[:, back_lanes + LANES :]
            extra = []
            for v in range(back_vregs):
                here = kz_back_ref[place_ref[1] ^ py, v] * by_z
                if v == 0:
                    here = here + by_y
                extra.append(here)
            extra = jnp.concatenate(extra, axis=1)
            for px in range(parts_x):
                re = slice(px * rows, px * rows + width_y)
                im = slice(px * rows + width_y, (px + 1) * rows)
                total = jnp.concatenate(
                    [value[re, :back_lanes] - extra[im], value[im, :back_lanes] + extra[re]], axis=0
                )
                out_refs[px * parts_y + py][dx] = total.astype(BF16)

    lax.fori_loop(0, PATCH // 2, section_back, 0, unroll=PLANE_UNROLL)


def back_groups(width_z):
    names = [{"a": "v", "g": "g"}[slot[0]] + slot[1] for slot in BACK_SLOTS]
    lanes = up_to(len(BACK_SLOTS) * width_z, LANES)
    groups = []
    for v in range(lanes // LANES):
        groups.append([n for slot, n in enumerate(names) if v in vregs_of(slot, width_z)])
    groups.append(["gz", "gx"])
    groups.append(["gy", "gx"])
    return groups


def back_table(width_z, length, parts_y):
    names = [{"a": "v", "g": "g"}[slot[0]] + slot[1] for slot in BACK_SLOTS]
    lanes = up_to(len(BACK_SLOTS) * width_z, LANES)
    groups = back_groups(width_z)
    order = box_order(length)

    def piece(slot, vreg, py, sign):
        modes, inside = lane_modes(slot, width_z, lanes, py * width_z)
        cut = slice(vreg * LANES, (vreg + 1) * LANES)
        cosine, sine = angles(order, modes[cut], length)
        keep = sign * inside[cut].astype(np.float32)[None, :]
        return np.concatenate([cosine * keep, -sine * keep], axis=1)

    ky_slots = {"gz": (BACK_SLOTS.index("ax"), 1.0), "gx": (BACK_SLOTS.index("az"), -1.0)}
    kz_slots = {"gy": (BACK_SLOTS.index("ax"), -1.0), "gx": (BACK_SLOTS.index("ay"), 1.0)}
    tables = []
    for py in range(parts_y):
        rows = []
        for v, group in enumerate(groups[:-2]):
            rows += [piece(names.index(n), v, py, 1.0) for n in group]
        for which, group in ((ky_slots, groups[-2]), (kz_slots, groups[-1])):
            for n in group:
                slot, sign = which[n]
                rows.append(sum(piece(slot, v, py, sign) for v in vregs_of(slot, width_z)))
        tables.append(np.concatenate(rows, axis=0))
    return jnp.asarray(np.stack(tables), BF16)


def out_table(slot, width_z, length, parts_y):
    lanes = (vregs_of(slot, width_z)[-1] + 1) * LANES
    order = box_order(length)
    tables = []
    for py in range(parts_y):
        modes, inside = lane_modes(slot, width_z, lanes, py * width_z)
        cosine, sine = angles(modes, order, length)
        keep = inside.astype(np.float32)[:, None]
        rows = []
        for value in (cosine, -sine):
            for v in vregs_of(slot, width_z):
                rows.append((value * keep)[v * LANES : (v + 1) * LANES])
        tables.append(np.concatenate(rows, axis=0))
    return jnp.asarray(np.stack(tables), BF16)


def physical(recv, place, ky_rows, kz_in, kz_back, tables, weights, grid_sizes, back_lanes):
    parts_x, parts_y, width_y, width_z, length = grid_sizes
    parts = parts_x * parts_y
    span, rows, in_lanes = recv[0].shape
    hid = weights[0].shape[0]
    feat = weights[0].shape[1]
    t_y, t_yb, z_tables, z_back = tables

    def whole(array):
        return pl.BlockSpec(array.shape, lambda i: (0,) * array.ndim)

    small = [ky_rows, kz_in, kz_back, t_y, t_yb, *weights, *z_tables, z_back]
    feat_pad = up_to(feat + 1, 2 * LANES)
    boxed = (length // LANES, 2, length // (2 * PATCH), 3 * PATCH * PATCH, LANES)
    flops = 2 * span * parts_y * (2 * length) * (parts_x * rows) * (in_lanes + LANES)
    flops += 2 * 5 * hid * feat * (span * length * length // PATCH**3)
    flops += 2 * span * length * length * length * (9 * 2 + 20)
    return pl.pallas_call(
        functools.partial(
            physical_kernel,
            parts_x=parts_x,
            parts_y=parts_y,
            width_y=width_y,
            width_z=width_z,
            length=length,
            back_lanes=back_lanes,
        ),
        grid=(span // PATCH,),
        in_specs=[pl.BlockSpec((PATCH, rows, in_lanes), lambda i: (i, 0, 0))] * parts
        + [pl.BlockSpec(memory_space=pltpu.SMEM)]
        + [whole(a) for a in small],
        out_specs=[pl.BlockSpec((PATCH, rows, back_lanes), lambda i: (i, 0, 0))] * parts
        + [
            pl.BlockSpec((hid, feat_pad), lambda i: (0, 0)),
            pl.BlockSpec((hid, feat), lambda i: (0, 0)),
        ],
        out_shape=[jax.ShapeDtypeStruct((span, rows, back_lanes), BF16)] * parts
        + [
            jax.ShapeDtypeStruct((hid, feat_pad), F32),
            jax.ShapeDtypeStruct((hid, feat), F32),
        ],
        scratch_shapes=[
            pltpu.VMEM((parts_y, PATCH, 2 * length, in_lanes + LANES), BF16),
            pltpu.VMEM(boxed, F32),
            pltpu.VMEM(boxed, F32),
            pltpu.VMEM((3, 3, PATCH, length, length), BF16),
            pltpu.VMEM(boxed, F32),
            pltpu.VMEM((parts_y, 2 * length, back_lanes + 2 * LANES), BF16),
        ],
        compiler_params=pltpu.CompilerParams(vmem_limit_bytes=58 * 2**20),
        cost_estimate=pl.CostEstimate(
            flops=flops, bytes_accessed=4 * parts * recv[0].size, transcendentals=0
        ),
        name="physical",
    )(*recv, place, *small)


def final_kernel(
    partner_ref,
    ky_ref,
    kz_ref,
    table_ref,
    base_ref,
    *refs,
    steps_in,
    block,
    width_y,
    width_z,
    length,
    first,
):
    out_ref, scratch, turned = refs[-3:]
    recv_refs = refs[:-3]
    parts = partner_ref.shape[0]
    planes = len(recv_refs) * steps_in
    step = pl.program_id(0)
    rows = 2 * width_y
    lanes = recv_refs[0].shape[2]

    @pl.when(step < steps_in)
    def _():
        for j, recv_ref in enumerate(recv_refs):
            source = partner_ref[j % parts]
            x = (j // parts * parts + source) * steps_in + step
            at = pl.multiple_of(x * rows, 8)
            value = recv_ref[0].astype(F32)
            for v in range(lanes // LANES):
                scratch[v, pl.ds(at, rows), :] = value[:, v * LANES : (v + 1) * LANES]

    @pl.when(step >= steps_in)
    def _():
        cutoff = float(length // 3)
        wave_z = kz_ref[...]
        counter = lax.broadcasted_iota(jnp.int32, wave_z.shape, 1)
        wave_x = jnp.where(counter < length // 2, counter, counter - length).astype(F32)
        plane = wave_x * wave_x + wave_z * wave_z
        inside = (jnp.abs(wave_x) <= cutoff) & (wave_z <= cutoff)
        weight = jnp.where(wave_z == 0.0, 1.0, 2.0).astype(F32)

        def one(k, carry):
            ky = (step - steps_in) * block + k
            pieces = []
            for v in range(lanes // LANES):
                parts_s = [
                    scratch[v, pl.ds(ky + s * width_y, planes, stride=rows), :] for s in range(2)
                ]
                pieces.append(jnp.concatenate(parts_s, axis=0))
            gathered = jnp.concatenate(pieces, axis=1).astype(BF16)
            turned[k % LAST_UNROLL] = dot_tn(gathered, table_ref[...])
            wave_y = ky_ref[ky]
            kept = jnp.where(inside & (jnp.abs(wave_y) <= cutoff), 1.0, 0.0).astype(F32)
            scale = kept * weight
            factor = jnp.exp(-NU_DT * (plane + wave_y * wave_y)) if first else 1.0

            def part(name, t):
                at = BACK_SLOTS.index(name) * width_z
                return turned[k % LAST_UNROLL, pl.ds(at, width_z), pl.ds(t * length, length)]

            for t in range(2):
                sign = -1.0 if t == 0 else 1.0
                ax = part("ax", t)
                ay = part("ay", t) - sign * wave_x * part("gz", 1 - t)
                az = part("az", t) + sign * wave_x * part("gy", 1 - t)
                for c, value in enumerate((ax, ay, az)):
                    out_ref[c, t, k] = factor * base_ref[c, t, k] + scale * value
            return carry

        lax.fori_loop(0, block, one, 0, unroll=LAST_UNROLL)


def finish(partners, ky, kz_col, table, base, received, first):
    _, _, width_y, width_z, length = base.shape
    span, rows, lanes = received[0].shape
    block = 8
    steps_in = span
    steps = steps_in + width_y // block
    spec = pl.BlockSpec(
        (3, 2, block, width_z, length), lambda i: (0, 0, jnp.maximum(i - steps_in, 0), 0, 0)
    )
    recv_spec = pl.BlockSpec((1, rows, lanes), lambda i: (jnp.minimum(i, steps_in - 1), 0, 0))
    return pl.pallas_call(
        functools.partial(
            final_kernel,
            steps_in=steps_in,
            block=block,
            width_y=width_y,
            width_z=width_z,
            length=length,
            first=first,
        ),
        grid=(steps,),
        in_specs=[
            pl.BlockSpec(memory_space=pltpu.SMEM),
            pl.BlockSpec(memory_space=pltpu.SMEM),
            pl.BlockSpec((width_z, length), lambda i: (0, 0)),
            pl.BlockSpec(table.shape, lambda i: (0, 0)),
            spec,
        ]
        + [recv_spec] * len(received),
        out_specs=spec,
        out_shape=jax.ShapeDtypeStruct(base.shape, F32),
        scratch_shapes=[
            pltpu.VMEM((lanes // LANES, len(received) * span * rows, LANES), F32),
            pltpu.VMEM((LAST_UNROLL, lanes, 2 * length), F32),
        ],
        compiler_params=pltpu.CompilerParams(vmem_limit_bytes=60 * 2**20),
        cost_estimate=pl.CostEstimate(
            flops=2 * width_y * lanes * table.size * 2,
            bytes_accessed=8 * base.size,
            transcendentals=0,
        ),
        name="finish",
    )(partners, ky, kz_col, table, base, *received)


def shards(state, cotangent, w_in, b_in, w_out):
    width_y, width_z, length = state.shape[2:]
    parts_x = lax.axis_size("px")
    parts_y = lax.axis_size("py")
    parts = parts_x * parts_y
    slab = length // parts
    chunks = MAX_CHUNKS
    while chunks > 1 and slab % (chunks * PATCH) != 0:
        chunks //= 2
    span = slab // chunks
    ky_count = width_y * parts_x
    hid, feat = w_in.shape

    own_x = lax.axis_index("px")
    own_y = lax.axis_index("py")
    own = own_x * parts_y + own_y
    partners = own ^ jnp.arange(parts, dtype=jnp.int32)
    partners_x = own_x ^ jnp.arange(parts_x, dtype=jnp.int32)
    local_y = jnp.arange(width_y, dtype=jnp.int32)
    ky_ids = own_x * width_y + local_y
    kz_ids = own_y * width_z + jnp.arange(width_z, dtype=jnp.int32)
    ky = signed(ky_ids, ky_count)
    kz_col = jnp.broadcast_to(kz_ids.astype(F32)[:, None], (width_z, length))

    everything = np.arange(length)
    cosine, sine = angles(everything, everything, length)
    both = np.stack(
        [np.concatenate([cosine, -sine], axis=1), np.concatenate([sine, cosine], axis=1)]
    )
    x_back = both.reshape(2, parts, chunks, span, 2 * length).transpose(2, 0, 1, 3, 4)
    x_rows = both.reshape(2, parts, chunks, span, 2 * length).transpose(1, 2, 0, 3, 4)
    x_rows = jnp.asarray(x_rows.reshape(parts, chunks, 2 * span, 2 * length), BF16)

    ky_modes = mode_ids(ky_count, length)
    cosine, sine = angles(everything, ky_modes, length)
    cosine = cosine.reshape(length, parts_x, width_y)
    sine = sine.reshape(length, parts_x, width_y)
    t_y = np.stack(
        [np.concatenate([cosine, -sine], axis=2), np.concatenate([sine, cosine], axis=2)]
    )
    t_yb = jnp.asarray(t_y.reshape(2 * length, parts_x, -1).transpose(1, 2, 0), BF16)
    t_y = jnp.asarray(t_y.reshape(2 * length, parts_x, -1), BF16)
    t_y = jnp.take(t_y, partners_x, axis=1).reshape(2 * length, -1)

    z_tables = [out_table(slot, width_z, length, parts_y) for slot in range(len(OUT_SLOTS))]
    z_tables.append(z_tables[0])
    z_back = back_table(width_z, length, parts_y)

    back_lanes = up_to(len(BACK_SLOTS) * width_z, LANES)
    ky_order = (partners_x[:, None] * width_y + local_y[None, :]).astype(jnp.int32)
    ky_rows = signed(ky_order, ky_count).reshape(parts_x, 1, width_y, 1)
    ky_rows = jnp.broadcast_to(ky_rows, (parts_x, 2, width_y, LANES)).reshape(-1, LANES)
    kz_in, kz_back = [], []
    for py in range(parts_y):
        modes, inside = lane_modes(0, width_z, LANES, py * width_z)
        kz_in.append(np.where(inside, modes, 0)[None, :])
        total = np.zeros((back_lanes,))
        for name in ("ax", "ay"):
            slot = BACK_SLOTS.index(name)
            modes, inside = lane_modes(slot, width_z, back_lanes, py * width_z)
            total = total + np.where(inside, modes, 0)
        kz_back.append(total.reshape(-1, 1, LANES))
    kz_in = jnp.asarray(np.stack(kz_in), F32)
    kz_back = jnp.asarray(np.stack(kz_back), F32)

    units = hid // parts

    def turn(weight):
        split = weight.reshape(parts, units, 3, PATCH, PATCH, PATCH)[partners]
        return split.transpose(0, 1, 5, 2, 3, 4).reshape(hid, feat)

    w_in_f = turn(w_in)
    w_out_t = turn(w_out.T)
    bias = b_in.reshape(parts, units)[partners].reshape(hid, 1)
    bias = jnp.broadcast_to(bias, (hid, LANES))
    weights = (w_in_f, w_in_f.T, w_out_t, bias)

    def exchange(arrays):
        moved = [arrays[0]]
        for k in range(1, parts):
            pairs = [(i, i ^ k) for i in range(parts)]
            moved.append(lax.ppermute(arrays[k], ("px", "py"), pairs))
        return moved

    spectra = make_spectra(ky, kz_col, state, cotangent)
    spectra = spectra.reshape(width_y, -1, 2 * length)
    arrived = []
    groups = ((0, 1), (1, 1), (2, 2)) if chunks == 4 else tuple((j, 1) for j in range(chunks))
    for first, count in groups:
        outs = along_x(partners, x_rows, spectra, first, count)
        for sent in outs:
            arrived.append(exchange(sent))
    place = jnp.stack([own_x, own_y]).astype(jnp.int32)
    grid_sizes = (parts_x, parts_y, width_y, width_z, length)
    tables = (t_y, t_yb, z_tables, z_back)
    returned = []
    grads = 0.0
    for recv in arrived:
        *sent, gin, gout = physical(
            recv, place, ky_rows, kz_in, kz_back, tables, weights, grid_sizes, back_lanes
        )
        returned.append(exchange(sent))
        grads = grads + jnp.concatenate([gin, gout], axis=1)
    grads = exchange([grads[k * units : (k + 1) * units] for k in range(parts)])
    grads = sum(grads)

    state_grad = cotangent
    ends = ((0, chunks - 1), (chunks - 1, chunks)) if chunks > 1 else ((0, chunks),)
    for j, (low, high) in enumerate(ends):
        received = [array for chunk in returned[low:high] for array in chunk]
        table = x_back[low:high].transpose(1, 0, 2, 3, 4).reshape(-1, 2 * length)
        table = jnp.asarray(table, BF16)
        state_grad = finish(partners, ky, kz_col, table, state_grad, received, j == 0)

    pad = up_to(feat + 1, 2 * LANES)

    def unturn(weight):
        split = weight.reshape(units, PATCH, 3, PATCH, PATCH)
        return split.transpose(0, 2, 3, 4, 1).reshape(units, feat)

    grad_in = unturn(grads[:, :feat])
    grad_bias = grads[:, feat][None, :]
    grad_out = FORCING * unturn(grads[:, pad:]).T
    return state_grad, grad_in, grad_out, grad_bias


def solution(mesh):
    return jax.shard_map(
        shards,
        mesh=mesh,
        in_specs=(
            P("rep", None, "px", "py", None),
            P("rep", None, "px", "py", None),
            P(),
            P(),
            P(),
        ),
        out_specs=(
            P("rep", None, "px", "py", None),
            P(("px", "py"), "rep"),
            P("rep", ("px", "py")),
            P("rep", ("px", "py")),
        ),
        check_vma=False,
    )
```
